32 devices in a mesh: shard: 16 (over z, x, core), task: 2 (over y).
Axes of the slice: x: 2, y: 2, z: 4, core: 2. Of those that a mesh axis runs over, the one named last changes fastest.
Arguments:
- task_deltas: bfloat16 [2, 4, 256, 16384], P('task', None, 'shard')
- rank_scores: int32 [2, 4, 256, 16384], P('task', None, 'shard'), may hold values from 0 to 1073741823
- keep_limits: int32 [2, 4, 8], P('task'), may hold values from 268435456 to 805306367
Outputs:
- merged: bfloat16 [4, 256, 16384], P(None, 'shard', 'task')
The draws below stay inside these ranges and needn't reach their ends.
All inputs are finite; a program needn't handle non-finite values.
Results may differ from the reference program's by a relative error of at most 0.0051.
Values may be sent and summed in bfloat16 or wider, within the bound.
No kernel may reach another device: no remote copies, remote signals or barrier semaphores. Data moves between devices by JAX's collectives and lax.ppermute only.
A program may use at most 64 MiB of HBM per device.

```python
import math
import jax
import jax.numpy as jnp
from jax import lax

EXPERTS = 8
FF = 16384
LAYERS = 4
ROWS = 32
TASKS = 2


def draw_task_deltas(key, part):
    key_base, key_column, key_row = jax.random.split(key, 3)
    row_total = EXPERTS * ROWS
    shape = (TASKS, LAYERS, row_total, FF)
    rising = 1.0 + 2.0 * jnp.arange(row_total, dtype=jnp.float32) / max(row_total - 1, 1)
    base = jax.random.normal(key_base, shape, jnp.float32)
    column = 0.03 * jnp.exp(jax.random.uniform(key_column, (TASKS, LAYERS, 1, FF), jnp.float32, 0.0, math.log(10.0)))
    row_scale = jnp.exp(jax.random.uniform(key_row, (TASKS, LAYERS, row_total, 1), jnp.float32, 0.0, math.log(10.0)))
    return (base * column * row_scale * rising[None, None, :, None]).astype(jnp.bfloat16)


def plant(result, stream_key, smallest, top_value):
    longest = result.shape.index(max(result.shape))
    spots = []
    for shift in (0, 1):
        where = [jax.random.randint(jax.random.fold_in(stream_key, axis), (), 0, length) for axis, length in enumerate(result.shape)]
        where[longest] = (where[longest] + shift) % result.shape[longest]
        spots.append(tuple(where))
    return result.at[spots[0]].set(smallest).at[spots[1]].set(top_value)


def setup_inputs(seed: int = 0) -> dict:
    key_list = jax.random.split(jax.random.key(seed), 4)
    return {
        "task_deltas": draw_task_deltas(jax.random.fold_in(key_list[3], 71), 0),
        "rank_scores": plant(jax.random.randint(key_list[1], (TASKS, LAYERS, EXPERTS * ROWS, FF), 0, 1073741824), jax.random.fold_in(key_list[1], 1), 0, 1073741823).astype(jnp.int32),
        "keep_limits": plant(jax.random.randint(key_list[2], (TASKS, LAYERS, EXPERTS), 268435456, 805306368), jax.random.fold_in(key_list[2], 1), 268435456, 805306367).astype(jnp.int32),
    }


def keep_probability(column_sums, grand_sums, row_total):
    column_mean = column_sums / row_total
    grand_mean = grand_sums / (EXPERTS * row_total * FF)
    return (0.2 + 0.7 * column_mean / (column_mean + grand_mean)).astype(jnp.bfloat16)


def reference(task_deltas, rank_scores, keep_limits):
    outputs = []
    for layer_at in range(LAYERS):
        change = task_deltas[:, layer_at].astype(jnp.float32).reshape(TASKS, EXPERTS, ROWS, FF)
        column_sums = jnp.sum(jnp.abs(change), axis=2)
        grand_sums = jnp.sum(column_sums, axis=(1, 2))
        rounded = lax.optimization_barrier(keep_probability(column_sums, grand_sums[:, None, None], ROWS))
        probability = rounded.astype(jnp.float32)
        scores = rank_scores[:, layer_at].reshape(TASKS, EXPERTS, ROWS, FF)
        limits = keep_limits[:, layer_at][:, :, None, None]
        retained = jnp.where(scores < limits, change / probability[:, :, None, :], jnp.float32(0.0))
        merged = jnp.sum(retained, axis=0).reshape(EXPERTS * ROWS, FF).astype(jnp.bfloat16)
        outputs.append(merged)
    return jnp.stack(outputs)
```

```python
import jax
import jax.numpy as jnp
from jax import lax
from jax.sharding import PartitionSpec as P

EXPERTS = 8
FF = 16384


def swapped(value, axis, bit):
    pairs = [(source, source ^ (1 << bit)) for source in range(lax.axis_size(axis))]
    return lax.ppermute(value, axis, pairs)


def shifted(value, axis, step):
    size = lax.axis_size(axis)
    return lax.ppermute(value, axis, [(source, (source + step) % size) for source in range(size)])


def inverse_probability(column_mean, grand_mean):
    return 1.0 / (0.2 + 0.7 * column_mean / (column_mean + grand_mean))


def on_device(task_deltas, rank_scores, keep_limits):
    shards, tasks = lax.axis_size("shard"), lax.axis_size("task")
    groups = shards // EXPERTS
    group_bits = groups.bit_length() - 1
    expert = lax.axis_index("shard") // groups
    task = lax.axis_index("task")
    layers, row_count, width = task_deltas.shape[1:]
    rows_whole = row_count * groups
    columns = width // tasks
    deltas, scores = task_deltas[0], rank_scores[0]
    limits = lax.dynamic_index_in_dim(keep_limits[0], expert, 1, keepdims=False)

    def own(value, step):
        return lax.dynamic_slice_in_dim(value, (task + step) % tasks * columns, columns, value.ndim - 1)

    def masked(layer, step):
        return jnp.where(own(scores[layer], step) < limits[layer], own(deltas[layer], step), jnp.bfloat16(0))

    arrived = [[shifted(masked(layer, step), "task", step) for layer in range(layers)] for step in range(1, tasks)]

    sums = jnp.sum(jnp.abs(deltas.astype(jnp.float32)), axis=1)
    for bit in range(group_bits):
        sums = sums + swapped(sums, "shard", bit)
    totals = jnp.sum(sums, axis=1)
    means = sums / rows_whole
    all_means = [own(means, 0)]
    all_totals = [totals]
    for step in range(1, tasks):
        all_means.append(shifted(own(means, step).astype(jnp.bfloat16), "task", step).astype(jnp.float32))
        all_totals.append(shifted(totals, "task", step))
    totals = jnp.stack(all_totals)
    for bit in range(group_bits, shards.bit_length() - 1):
        totals = totals + swapped(totals, "shard", bit)
    grand = totals / (EXPERTS * rows_whole * FF)

    results = []
    for layer in range(layers):
        merged = masked(layer, 0).astype(jnp.float32) * inverse_probability(all_means[0][layer], grand[0, layer])
        for step in range(1, tasks):
            scale = inverse_probability(all_means[step][layer], grand[step, layer])
            merged = merged + arrived[step - 1][layer].astype(jnp.float32) * scale
        results.append(merged.astype(jnp.bfloat16))
    return jnp.stack(results)


def solution(mesh):
    return jax.shard_map(
        on_device,
        mesh=mesh,
        in_specs=(
            P("task", None, "shard", None),
            P("task", None, "shard", None),
            P("task", None, None),
        ),
        out_specs=P(None, "shard", "task"),
        check_vma=False,
    )
```

```python
import functools

import jax
import jax.numpy as jnp
from jax import lax
from jax.experimental import pallas as pl
from jax.experimental.pallas import tpu as pltpu
from jax.sharding import PartitionSpec as P


EXPERTS = 8
FF = 16384
LANES = 128
BLOCK = 1024

ANY = pl.BlockSpec(memory_space=pl.ANY)
VMEM = pl.BlockSpec(memory_space=pltpu.VMEM)


def crossed(value, axis, mask):
    return lax.ppermute(value, axis, [(source, source ^ mask) for source in range(lax.axis_size(axis))])


def swapped(value, axis, bit):
    return crossed(value, axis, 1 << bit)


def shifted(value, axis, step):
    size = lax.axis_size(axis)
    return lax.ppermute(value, axis, [(source, (source + step) % size) for source in range(size)])


def column_start(step, columns):
    tasks = lax.axis_size("task")
    return lax.rem(lax.axis_index("task") + step, tasks) * columns


def own_expert():
    return lax.axis_index("shard") // (lax.axis_size("shard") // EXPERTS)


def blocks(width, body):
    block = min(BLOCK, width)

    @pl.loop(0, width // block)
    def _(at):
        body(pl.multiple_of(at * block, block), block)


def mask_block(deltas, scores, limit):
    return jnp.where(scores < limit, deltas.astype(jnp.float32), 0.0).astype(jnp.bfloat16)


def first_kernel(limits, deltas, scores, *refs):
    tasks = lax.axis_size("task")
    outs = refs[: tasks - 1]
    limit_buf, delta_buf, score_buf, sems = refs[tasks - 1 :]
    columns = outs[0].shape[1]
    copies = [pltpu.make_async_copy(limits, limit_buf, sems.at[0])]
    for step in range(1, tasks):
        source = pl.ds(pl.multiple_of(column_start(step, columns), LANES), columns)
        copies.append(pltpu.make_async_copy(scores.at[0, 0, :, source], score_buf.at[step - 1], sems.at[2 * step - 1]))
        copies.append(pltpu.make_async_copy(deltas.at[0, 0, :, source], delta_buf.at[step - 1], sems.at[2 * step]))
    for copy in copies:
        copy.start()
    copies[0].wait()
    limit = limit_buf[0, 0, own_expert()]
    for step in range(1, tasks):
        copies[2 * step - 1].wait()
        copies[2 * step].wait()
        out = outs[step - 1]

        def body(at, block):
            where = pl.ds(at, block)
            out[:, where] = mask_block(delta_buf[step - 1, :, where], score_buf[step - 1, :, where], limit)

        blocks(columns, body)


def rest_kernel(limits, deltas, scores, *refs):
    tasks = lax.axis_size("task")
    layers, rows, width = deltas.shape[1:]
    columns = width // tasks
    half = columns // 2
    block = min(BLOCK, half)
    places = half // block
    folded = 2 * layers
    groups = lax.axis_size("shard") // EXPERTS
    sent = [refs[(layer - 1) * (tasks - 1) : layer * (tasks - 1)] for layer in range(1, layers)]
    refs = refs[(layers - 1) * (tasks - 1) :]
    packs, refs = refs[:tasks], refs[tasks:]
    own, limit_buf, delta_buf, score_buf, sems = refs
    limit_copy = pltpu.make_async_copy(limits, limit_buf, sems.at[0])
    limit_copy.start()
    work = [(step, place) for step in [*range(1, tasks), 0] for place in range(places)]
    copies = []
    for step, place in work:
        start = column_start(step, columns)
        pending = []
        for part in range(2):
            source = pl.ds(pl.multiple_of(start + part * half + place * block, LANES), block)
            skip = 1 if step else 0
            at = 1 + 4 * len(copies) + 2 * part
            pending.append(pltpu.make_async_copy(
                deltas.at[0, :, :, source], delta_buf.at[len(copies), part], sems.at[at]))
            pending.append(pltpu.make_async_copy(
                scores.at[0, skip:, :, source], score_buf.at[len(copies), part, skip:], sems.at[at + 1]))
        for copy in pending:
            copy.start()
        copies.append(pending)
    shape = (folded, folded * rows)
    taken = lax.broadcasted_iota(jnp.int32, shape, 1) // rows == lax.broadcasted_iota(jnp.int32, shape, 0)
    selector = jnp.where(taken, 1.0, 0.0).astype(jnp.bfloat16)
    totals = jnp.zeros((folded, LANES), jnp.float32)
    limit_copy.wait()
    chosen = [limit_buf[0, layer, own_expert()] for layer in range(layers)]
    for at, (step, place) in enumerate(work):
        for copy in copies[at]:
            copy.wait()
        change = delta_buf[at].reshape(folded * rows, block)
        sums = jnp.dot(selector, jnp.abs(change), preferred_element_type=jnp.float32)
        means = sums * (1.0 / (rows * groups))
        packs[step][:, place * block : (place + 1) * block] = means.astype(jnp.bfloat16)
        for tile in range(0, block, LANES):
            totals = totals + means[:, tile : tile + LANES]
        for part in range(2):
            target = pl.ds(part * half + place * block, block)
            for layer in range(layers):
                if step and not layer:
                    continue
                kept = mask_block(delta_buf[at, part, layer], score_buf[at, part, layer], chosen[layer])
                if step:
                    sent[layer - 1][step - 1][:, target] = kept
                else:
                    own[layer, :, target] = kept
    high = totals.astype(jnp.bfloat16)
    low = (totals - high.astype(jnp.float32)).astype(jnp.bfloat16)
    for step in range(tasks):
        packs[step][:, half : half + LANES] = high
        packs[step][:, half + LANES :] = low


def join_kernel(*refs):
    tasks = lax.axis_size("task")
    means, totals = refs[2 * tasks :]
    half = means.shape[2]
    for step in range(tasks):
        mine = refs[2 * step][...].astype(jnp.float32)
        theirs = refs[2 * step + 1][...].astype(jnp.float32)
        both = mine + theirs
        means[step] = both[:, :half]
        totals[step] = both[:, half : half + LANES] + both[:, half + LANES :]


def scale_kernel(means, totals, scales):
    tasks, folded, _ = means.shape
    for step in range(tasks):
        total = jnp.sum(totals[step], axis=1, keepdims=True)
        total = total + jnp.concatenate([total[folded // 2 :], total[: folded // 2]], axis=0)
        grand = total * (1.0 / (EXPERTS * FF))
        mean = means[step]
        rounded = (0.2 + 0.7 * mean / (mean + grand)).astype(jnp.bfloat16)
        scales[step] = 1.0 / rounded.astype(jnp.float32)


def merge_layers(picked, tasks, aliased, scales, own, *refs):
    half = scales.shape[2]
    layers = own.shape[0]
    arrived = refs[: len(picked) * (tasks - 1)]
    refs = refs[len(arrived) + aliased :]
    out, buf, sems = refs
    copies = []
    for place, layer in enumerate(picked):
        for part in range(2):
            row = part * layers + layer

            def body(at, block):
                narrow = pl.ds(at, block)
                where = pl.ds(pl.multiple_of(part * half + at, LANES), block)
                merged = own[layer, :, where].astype(jnp.float32) * scales[0, row : row + 1, narrow]
                for step in range(1, tasks):
                    other = arrived[place * (tasks - 1) + step - 1][:, where].astype(jnp.float32)
                    merged = merged + other * scales[step, row : row + 1, narrow]
                buf[place, :, where] = merged.astype(jnp.bfloat16)

            blocks(half, body)
        copies.append(pltpu.make_async_copy(buf.at[place], out.at[layer], sems.at[place]))
        copies[-1].start()
    for copy in copies:
        copy.wait()


def cost(flops, moved):
    return pl.CostEstimate(flops=flops, bytes_accessed=moved, transcendentals=0)


def on_chip(value):
    return pltpu.with_memory_space_constraint(value, pltpu.VMEM)


def merge_all(task_deltas, rank_scores, keep_limits):
    shards, tasks = lax.axis_size("shard"), lax.axis_size("task")
    groups = shards // EXPERTS
    group_bits = groups.bit_length() - 1
    layers, rows, width = task_deltas.shape[1:]
    columns = width // tasks
    half = columns // 2
    block = min(BLOCK, half)
    bf16, f32 = jnp.bfloat16, jnp.float32
    slab = pltpu.VMEM((rows, columns), bf16)

    first = pl.pallas_call(
        first_kernel,
        out_shape=[slab] * (tasks - 1),
        in_specs=[ANY] * 3,
        out_specs=[VMEM] * (tasks - 1),
        scratch_shapes=[
            pltpu.SMEM(keep_limits.shape, jnp.int32),
            pltpu.VMEM((tasks - 1, rows, columns), bf16),
            pltpu.VMEM((tasks - 1, rows, columns), jnp.int32),
            pltpu.SemaphoreType.DMA((2 * tasks - 1,)),
        ],
        cost_estimate=cost(10**6, 6 * rows * columns),
        name="first",
    )(keep_limits, task_deltas, rank_scores)
    arrived = [[shifted(first[step - 1], "task", step) for step in range(1, tasks)]]

    rest = pl.pallas_call(
        rest_kernel,
        out_shape=[slab] * ((layers - 1) * (tasks - 1))
        + [pltpu.VMEM((2 * layers, half + 2 * LANES), bf16)] * tasks
        + [pltpu.VMEM((layers, rows, columns), bf16)],
        in_specs=[ANY] * 3,
        out_specs=[VMEM] * ((layers - 1) * (tasks - 1) + tasks + 1),
        scratch_shapes=[
            pltpu.SMEM(keep_limits.shape, jnp.int32),
            pltpu.VMEM((tasks * half // block, 2, layers, rows, block), bf16),
            pltpu.VMEM((tasks * half // block, 2, layers, rows, block), jnp.int32),
            pltpu.SemaphoreType.DMA((4 * tasks * half // block + 1,)),
        ],
        cost_estimate=cost(10**7, 6 * layers * rows * width),
        name="rest",
    )(keep_limits, task_deltas, rank_scores)
    sent, packs, own = rest[: (layers - 1) * (tasks - 1)], rest[-tasks - 1 : -1], rest[-1]

    pairs = [packs[0], swapped(packs[0], "shard", 0)]
    for step in range(1, tasks):
        arrival = shifted(packs[step], "task", step)
        pairs += [arrival, swapped(arrival, "shard", 0)]
    for layer in range(1, layers):
        at = (layer - 1) * (tasks - 1)
        arrived.append([shifted(sent[at + step - 1], "task", step) for step in range(1, tasks)])

    means, totals = pl.pallas_call(
        join_kernel,
        out_shape=[pltpu.VMEM((tasks, 2 * layers, half), f32), pltpu.VMEM((tasks, 2 * layers, LANES), f32)],
        in_specs=[VMEM] * (2 * tasks),
        out_specs=[VMEM] * 2,
        cost_estimate=cost(10**6, 8 * tasks * layers * half),
        name="join",
    )(*[on_chip(pair) for pair in pairs])
    for bit in range(1, group_bits):
        means = means + swapped(means, "shard", bit)
        totals = totals + swapped(totals, "shard", bit)
    bits = [*range(group_bits, shards.bit_length() - 1)]
    for turn in (bits[:1], bits[1:]):
        masks = [0]
        for bit in turn:
            masks += [mask + (1 << bit) for mask in masks]
        totals = sum([crossed(totals, "shard", mask) for mask in masks[1:]], totals)

    scales = pl.pallas_call(
        scale_kernel,
        out_shape=pltpu.VMEM((tasks, 2 * layers, half), f32),
        in_specs=[VMEM] * 2,
        out_specs=VMEM,
        cost_estimate=cost(10**6, 8 * tasks * layers * half),
        name="scale",
    )(on_chip(means), on_chip(totals))

    out = None
    for picked in ([*range(layers - 1)], [layers - 1]):
        extra = [] if out is None else [out]
        arrivals = [on_chip(arrived[layer][step]) for layer in picked for step in range(tasks - 1)]
        out = pl.pallas_call(
            functools.partial(merge_layers, picked, tasks, len(extra)),
            out_shape=jax.ShapeDtypeStruct((layers, rows, columns), bf16),
            in_specs=[VMEM] * (2 + len(arrivals)) + [ANY] * len(extra),
            out_specs=ANY,
            scratch_shapes=[pltpu.VMEM((len(picked), rows, columns), bf16), pltpu.SemaphoreType.DMA((len(picked),))],
            input_output_aliases={2 + len(arrivals): 0} if extra else {},
            cost_estimate=cost(10**6, 6 * len(picked) * rows * columns),
            name="merge" if out is None else "merge_last",
        )(on_chip(scales), on_chip(own), *arrivals, *extra)
    return out


def solution(mesh):
    return jax.shard_map(
        merge_all,
        mesh=mesh,
        in_specs=(
            P("task", None, "shard", None),
            P("task", None, "shard", None),
            P("task", None, None),
        ),
        out_specs=P(None, "shard", "task"),
        check_vma=False,
    )
```

```python
import functools
import math

import jax
import jax.numpy as jnp
from jax import lax
from jax.experimental import pallas as pl
from jax.experimental.pallas import tpu as pltpu
from jax.sharding import PartitionSpec as P


EXPERTS = 8
FF = 16384
LANES = 128
BLOCK = 1024
PIECES = 4
GRANT = 16 * 2**20

ANY = pl.BlockSpec(memory_space=pl.ANY)
HBM = pl.BlockSpec(memory_space=pltpu.HBM)
VMEM = pl.BlockSpec(memory_space=pltpu.VMEM)


def crossed(value, axis, mask):
    return lax.ppermute(value, axis, [(source, source ^ mask) for source in range(lax.axis_size(axis))])


def swapped(value, axis, bit):
    return crossed(value, axis, 1 << bit)


def shifted(value, step):
    size = lax.axis_size("task")
    return lax.ppermute(value, "task", [(source, (source + step) % size) for source in range(size)])


def column_start(step, columns):
    tasks = lax.axis_size("task")
    return lax.rem(lax.axis_index("task") + step, tasks) * columns


def own_expert():
    return lax.axis_index("shard") // (lax.axis_size("shard") // EXPERTS)


def blocks(width, body):
    block = math.gcd(BLOCK, width)

    @pl.loop(0, width // block)
    def _(at):
        body(pl.multiple_of(at * block, block), block)


def chunk_plan(layers):
    last = layers - 1
    return [[(0, 0, 4)], [(layer, 0, 4) for layer in range(1, last)], [(last, 0, 3)], [(last, 3, 4)]]


def chunk_width(chunk, columns):
    return sum(end - begin for _, begin, end in chunk) * columns // 4


def mask_block(deltas, scores, limit):
    return jnp.where(scores < limit, deltas.astype(jnp.float32), 0.0).astype(jnp.bfloat16)


def first_kernel(limits, deltas, scores, *refs):
    tasks = lax.axis_size("task")
    outs = refs[: tasks - 1]
    limit_buf, delta_buf, score_buf, sems = refs[tasks - 1 :]
    columns = outs[0].shape[1]
    block = columns // PIECES
    limit_copy = pltpu.make_async_copy(limits, limit_buf, sems.at[0])
    limit_copy.start()
    work = [(step, piece) for step in range(1, tasks) for piece in range(PIECES)]
    copies = []
    for at, (step, piece) in enumerate(work):
        source = pl.ds(pl.multiple_of(column_start(step, columns) + piece * block, LANES), block)
        target = pl.ds(piece * block, block)
        copies.append([
            pltpu.make_async_copy(scores.at[0, 0, :, source], score_buf.at[step - 1, :, target], sems.at[2 * at + 1]),
            pltpu.make_async_copy(deltas.at[0, 0, :, source], delta_buf.at[step - 1, :, target], sems.at[2 * at + 2]),
        ])
        for copy in copies[-1]:
            copy.start()
    limit_copy.wait()
    limit = limit_buf[0, 0, own_expert()]
    for at, (step, piece) in enumerate(work):
        for copy in copies[at]:
            copy.wait()
        where = pl.ds(piece * block, block)
        outs[step - 1][:, where] = mask_block(delta_buf[step - 1, :, where], score_buf[step - 1, :, where], limit)


def row_sums(changes):
    values = [change.astype(jnp.float32) for change in changes]
    values = [sum(value[at : at + 8] for at in range(8, value.shape[0], 8)) + value[:8] for value in values]
    if len(values) != 8:
        return jnp.concatenate([jnp.sum(value, axis=0, keepdims=True) for value in values], axis=0)
    lane = lax.broadcasted_iota(jnp.int32, values[0].shape, 0)
    for shift in (4, 2, 1):
        low = lane % (2 * shift) < shift
        values = [
            jnp.where(low, one + pltpu.roll(one, 8 - shift, 0), two + pltpu.roll(two, shift, 0))
            for one, two in zip(values[:shift], values[shift:])
        ]
    return values[0]


def sums_kernel(deltas, copied, packs, sems):
    tasks, folded, packed = packs.shape
    half = packed - 2 * LANES
    layers, rows, _ = copied.shape
    columns = 2 * half
    block = min(BLOCK, half)
    places = half // block
    groups = lax.axis_size("shard") // EXPERTS
    work = [(step, place) for step in range(tasks) for place in range(places)]
    copies = []
    sources = []
    for step, place in work:
        start = column_start(step, columns) + place * block
        sources.append([pl.ds(pl.multiple_of(start + part * half, LANES), block) for part in range(2)])
        copies.append([
            pltpu.make_async_copy(deltas.at[0, :, :, source], copied.at[:, :, source], sems.at[2 * len(copies) + part])
            for part, source in enumerate(sources[-1])
        ])
        for copy in copies[-1]:
            copy.start()
    totals = jnp.zeros((folded, LANES), jnp.float32)
    for at, (step, place) in enumerate(work):
        for copy in copies[at]:
            copy.wait()
        sums = row_sums([jnp.abs(copied[layer, :, source]) for source in sources[at] for layer in range(layers)])
        means = sums * (1.0 / (rows * groups))
        packs[step, :, place * block : (place + 1) * block] = means.astype(jnp.bfloat16)
        for tile in range(0, block, LANES):
            totals = totals + means[:, tile : tile + LANES]
    for step in range(tasks):
        store_split(packs.at[step], totals)


def store_split(pack, totals):
    half = pack.shape[1] - 2 * LANES
    high = totals.astype(jnp.bfloat16)
    pack[:, half : half + LANES] = high
    pack[:, half + LANES :] = (totals - high.astype(jnp.float32)).astype(jnp.bfloat16)


def mask_kernel(chunks, own_layers, limits, scores, copied, *refs):
    tasks = lax.axis_size("task")
    _, _, width = copied.shape
    columns = width // tasks
    count = len(chunks) * (tasks - 1)
    sent, refs = refs[:count], refs[count:]
    if own_layers:
        own, refs = refs[0], refs[1:]
    limit_buf, score_buf, sems = refs
    limit_copy = pltpu.make_async_copy(limits, limit_buf, sems.at[0])
    limit_copy.start()
    work = []
    for at, chunk in enumerate(chunks):
        for step in range(1, tasks):
            offset = 0
            for layer, begin, end in chunk:
                size = (end - begin) * columns // 4
                work.append((sent[at * (tasks - 1) + step - 1], offset, layer, step, begin * columns // 4, size))
                offset += size
    work += [(own.at[layer], 0, layer, 0, 0, columns) for layer in own_layers]
    copies = []
    for at, (_, _, layer, step, begin, size) in enumerate(work):
        source = pl.ds(pl.multiple_of(column_start(step, columns) + begin, LANES), size)
        copies.append(pltpu.make_async_copy(scores.at[0, layer, :, source], score_buf.at[at, :, :size], sems.at[at + 1]))
        copies[-1].start()
    limit_copy.wait()
    for at, (target, offset, layer, step, begin, size) in enumerate(work):
        start = column_start(step, columns) + begin
        limit = limit_buf[0, layer, own_expert()]
        copies[at].wait()

        def body(place, block):
            change = copied[layer, :, pl.ds(pl.multiple_of(start + place, LANES), block)]
            kept = mask_block(change, score_buf[at, :, pl.ds(place, block)], limit)
            target[:, pl.ds(pl.multiple_of(offset + place, LANES), block)] = kept

        blocks(size, body)


def slot_lanes(width):
    return pl.ds(pl.multiple_of(lax.rem(lax.axis_index("shard"), 2) * width, LANES), width)


def pair_kernel(mine, theirs, means, totals, *refs):
    packs, both_buf = refs[:-1], refs[-1]
    tasks, _, packed = mine.shape
    half = packed - 2 * LANES
    both = mine[...].astype(jnp.float32) + theirs[...].astype(jnp.float32)
    both_buf[...] = both
    means[...] = both[0, :, :half]
    total = both[0, :, half : half + LANES] + both[0, :, half + LANES :]
    totals[...] = total
    for step in range(1, tasks):
        packs[step - 1][:, : half // 2] = both_buf[step, :, slot_lanes(half // 2)].astype(jnp.bfloat16)
        store_split(packs[step - 1], total)


def join_kernel(own_means, own_totals, *refs):
    tasks = lax.axis_size("task")
    means, totals = refs[2 * tasks - 2 :]
    half = means.shape[2]
    quarter = half // 2
    means[0] = own_means[...]
    totals[0] = own_totals[...]
    other = lax.rem(lax.axis_index("shard") + 1, 2) * quarter
    for step in range(1, tasks):
        mine, theirs = refs[2 * step - 2 : 2 * step]
        means[step, :, slot_lanes(quarter)] = mine[:, :quarter].astype(jnp.float32)
        means[step, :, pl.ds(pl.multiple_of(other, LANES), quarter)] = theirs[:, :quarter].astype(jnp.float32)
        both = mine[:, quarter:].astype(jnp.float32)
        totals[step] = both[:, :LANES] + both[:, LANES:]


def scale_kernel(means, totals, scales):
    tasks, folded, _ = means.shape
    for step in range(tasks):
        total = jnp.sum(totals[step], axis=1, keepdims=True)
        total = total + jnp.concatenate([total[folded // 2 :], total[: folded // 2]], axis=0)
        grand = total * (1.0 / (EXPERTS * FF))
        mean = means[step]
        rounded = (0.2 + 0.7 * mean / (mean + grand)).astype(jnp.bfloat16)
        scales[step] = 1.0 / rounded.astype(jnp.float32)


def merge_kernel(chunk, tasks, aliased, scales, own, *refs):
    half = scales.shape[2]
    layers = own.shape[0]
    columns = 2 * half
    arrived = refs[: tasks - 1]
    out, buf, sems = refs[tasks - 1 + aliased :]
    pieces = []
    offset = 0
    for layer, begin, end in chunk:
        for part in range(2):
            low, high = [min(max(at * columns // 4 - part * half, 0), half) for at in (begin, end)]
            if high > low:
                pieces.append((layer, part, low, high - low, offset))
                offset += high - low
    copies = []
    for at, (layer, part, low, size, offset) in enumerate(pieces):
        row = part * layers + layer

        def body(place, block):
            narrow = pl.ds(pl.multiple_of(low + place, LANES), block)
            source = pl.ds(pl.multiple_of(part * half + low + place, LANES), block)
            target = pl.ds(pl.multiple_of(offset + place, LANES), block)
            merged = own[layer, :, source].astype(jnp.float32) * scales[0, row : row + 1, narrow]
            for step in range(1, tasks):
                other = arrived[step - 1][:, target].astype(jnp.float32)
                merged = merged + other * scales[step, row : row + 1, narrow]
            buf[:, target] = merged.astype(jnp.bfloat16)

        blocks(size, body)
        copies.append(pltpu.make_async_copy(
            buf.at[:, pl.ds(offset, size)], out.at[layer, :, pl.ds(part * half + low, size)], sems.at[at]))
        copies[-1].start()
    for copy in copies:
        copy.wait()


def cost(flops, moved):
    return pl.CostEstimate(flops=flops, bytes_accessed=moved, transcendentals=0)


def on_chip(value):
    return pltpu.with_memory_space_constraint(value, pltpu.VMEM)


def merge_all(task_deltas, rank_scores, keep_limits):
    shards, tasks = lax.axis_size("shard"), lax.axis_size("task")
    groups = shards // EXPERTS
    group_bits = groups.bit_length() - 1
    layers, rows, width = task_deltas.shape[1:]
    columns = width // tasks
    half = columns // 2
    block = min(BLOCK, half)
    bf16, f32 = jnp.bfloat16, jnp.float32
    plan = chunk_plan(layers)
    slabs = [pltpu.VMEM((rows, chunk_width(chunk, columns)), bf16) for chunk in plan]

    task_deltas, rank_scores, keep_limits = [
        pltpu.with_memory_space_constraint(value, pltpu.HBM) for value in (task_deltas, rank_scores, keep_limits)
    ]
    first = pl.pallas_call(
        first_kernel,
        out_shape=[slabs[0]] * (tasks - 1),
        in_specs=[HBM] * 3,
        out_specs=[VMEM] * (tasks - 1),
        scratch_shapes=[
            pltpu.SMEM(keep_limits.shape, jnp.int32),
            pltpu.VMEM((tasks - 1, rows, columns), bf16),
            pltpu.VMEM((tasks - 1, rows, columns), jnp.int32),
            pltpu.SemaphoreType.DMA((2 * PIECES * (tasks - 1) + 1,)),
        ],
        compiler_params=pltpu.CompilerParams(vmem_limit_bytes=GRANT),
        cost_estimate=cost(10**6, 6 * rows * columns),
        name="first",
    )(keep_limits, task_deltas, rank_scores)
    arrived = [[shifted(first[step - 1], step) for step in range(1, tasks)]]

    pack = (2 * layers, half + 2 * LANES)
    copied, packs = pl.pallas_call(
        sums_kernel,
        out_shape=[pltpu.VMEM((layers, rows, width), bf16), pltpu.VMEM((tasks, *pack), bf16)],
        in_specs=[HBM],
        out_specs=[VMEM] * 2,
        scratch_shapes=[pltpu.SemaphoreType.DMA((2 * tasks * half // block,))],
        compiler_params=pltpu.CompilerParams(vmem_limit_bytes=GRANT),
        cost_estimate=cost(10**7, 2 * layers * rows * width),
        name="sums",
    )(task_deltas)

    def masks(places, own_layers):
        chunks = [plan[place] for place in places]
        shapes = [slabs[place] for place in places for _ in range(1, tasks)]
        shapes += [pltpu.VMEM((layers, rows, columns), bf16)] * bool(own_layers)
        pieces = sum(len(chunk) for chunk in chunks) * (tasks - 1) + len(own_layers)
        return pl.pallas_call(
            functools.partial(mask_kernel, chunks, own_layers),
            out_shape=shapes,
            in_specs=[HBM] * 2 + [VMEM],
            out_specs=[VMEM] * len(shapes),
            scratch_shapes=[
                pltpu.SMEM(keep_limits.shape, jnp.int32),
                pltpu.VMEM((pieces, rows, columns), jnp.int32),
                pltpu.SemaphoreType.DMA((pieces + 1,)),
            ],
            compiler_params=pltpu.CompilerParams(vmem_limit_bytes=GRANT),
            cost_estimate=cost(10**7, 6 * pieces * rows * columns),
            name="masks",
        )(keep_limits, rank_scores, on_chip(copied))

    for bit in range(1, group_bits):
        packs = packs.astype(f32) + swapped(packs, "shard", bit).astype(f32)
    theirs = swapped(packs, "shard", 0)
    sent = [*masks([1], [])]
    means, totals, *packs = pl.pallas_call(
        pair_kernel,
        out_shape=[pltpu.VMEM((2 * layers, half), f32), pltpu.VMEM((2 * layers, LANES), f32)]
        + [pltpu.VMEM((2 * layers, half // 2 + 2 * LANES), bf16)] * (tasks - 1),
        in_specs=[VMEM] * 2,
        out_specs=[VMEM] * (tasks + 1),
        scratch_shapes=[pltpu.VMEM((tasks, *pack), f32)],
        compiler_params=pltpu.CompilerParams(vmem_limit_bytes=GRANT),
        cost_estimate=cost(10**6, 8 * tasks * layers * half),
        name="pair",
    )(on_chip(packs), on_chip(theirs))
    arrivals = [shifted(packs[step - 1], step) for step in range(1, tasks)]
    arrived.append([shifted(sent[step - 1], step) for step in range(1, tasks)])
    sent += masks([*range(2, len(plan))], [])
    (own,) = masks([], [*range(layers)])
    pairs = []
    for arrival in arrivals:
        pairs += [arrival, swapped(arrival, "shard", 0)]
    for place in range(2, len(plan)):
        at = (place - 1) * (tasks - 1)
        arrived.append([shifted(sent[at + step - 1], step) for step in range(1, tasks)])

    means, totals = pl.pallas_call(
        join_kernel,
        out_shape=[pltpu.VMEM((tasks, 2 * layers, half), f32), pltpu.VMEM((tasks, 2 * layers, LANES), f32)],
        in_specs=[VMEM] * (2 * tasks),
        out_specs=[VMEM] * 2,
        compiler_params=pltpu.CompilerParams(vmem_limit_bytes=GRANT),
        cost_estimate=cost(10**6, 8 * tasks * layers * half),
        name="join",
    )(on_chip(means), on_chip(totals), *[on_chip(value) for value in pairs])
    for bit in range(group_bits, shards.bit_length() - 1):
        totals = totals + swapped(totals, "shard", bit)

    scales = pl.pallas_call(
        scale_kernel,
        out_shape=pltpu.VMEM((tasks, 2 * layers, half), f32),
        in_specs=[VMEM] * 2,
        out_specs=VMEM,
        compiler_params=pltpu.CompilerParams(vmem_limit_bytes=GRANT),
        cost_estimate=cost(10**6, 8 * tasks * layers * half),
        name="scale",
    )(on_chip(means), on_chip(totals))

    out = None
    for chunk, pieces in zip(plan, arrived):
        extra = [] if out is None else [out]
        out = pl.pallas_call(
            functools.partial(merge_kernel, chunk, tasks, len(extra)),
            out_shape=jax.ShapeDtypeStruct((layers, rows, columns), bf16),
            in_specs=[VMEM] * (1 + tasks) + [ANY] * len(extra),
            out_specs=ANY,
            scratch_shapes=[
                pltpu.VMEM((rows, chunk_width(chunk, columns)), bf16),
                pltpu.SemaphoreType.DMA((2 * len(chunk),)),
            ],
            input_output_aliases={1 + tasks: 0} if extra else {},
            compiler_params=pltpu.CompilerParams(vmem_limit_bytes=GRANT),
            cost_estimate=cost(10**6, 6 * rows * chunk_width(chunk, columns)),
            name="merge",
        )(on_chip(scales), on_chip(own), *[on_chip(piece) for piece in pieces], *extra)
    return out


def solution(mesh):
    return jax.shard_map(
        merge_all,
        mesh=mesh,
        in_specs=(
            P("task", None, "shard", None),
            P("task", None, "shard", None),
            P("task", None, None),
        ),
        out_specs=P(None, "shard", "task"),
        check_vma=False,
    )
```

```python
import functools
import math

import jax
import jax.numpy as jnp
from jax import lax
from jax.experimental import pallas as pl
from jax.experimental.pallas import tpu as pltpu
from jax.sharding import PartitionSpec as P


EXPERTS = 8
FF = 16384
LANES = 128
BLOCK = 1024
PIECES = 1
GRANT = 16 * 2**20

ANY = pl.BlockSpec(memory_space=pl.ANY)
HBM = pl.BlockSpec(memory_space=pltpu.HBM)
VMEM = pl.BlockSpec(memory_space=pltpu.VMEM)


def crossed(value, axis, mask):
    return lax.ppermute(value, axis, [(source, source ^ mask) for source in range(lax.axis_size(axis))])


def swapped(value, axis, bit):
    return crossed(value, axis, 1 << bit)


def shifted(value, step):
    size = lax.axis_size("task")
    return lax.ppermute(value, "task", [(source, (source + step) % size) for source in range(size)])


def column_start(step, columns):
    tasks = lax.axis_size("task")
    return lax.rem(lax.axis_index("task") + step, tasks) * columns


def own_expert():
    return lax.axis_index("shard") // (lax.axis_size("shard") // EXPERTS)


def blocks(width, body):
    block = math.gcd(BLOCK, width)

    @pl.loop(0, width // block)
    def _(at):
        body(pl.multiple_of(at * block, block), block)


def chunk_plan(layers):
    last = layers - 1
    return [[(0, 0, 4)], [(layer, 0, 4) for layer in range(1, last)], [(last, 0, 3)], [(last, 3, 4)]]


def chunk_width(chunk, columns):
    return sum(end - begin for _, begin, end in chunk) * columns // 4


def mask_block(deltas, scores, limit):
    return jnp.where(scores < limit, deltas.astype(jnp.float32), 0.0).astype(jnp.bfloat16)


def first_kernel(limits, deltas, scores, *refs):
    tasks = lax.axis_size("task")
    outs = refs[: tasks - 1]
    limit_buf, delta_buf, score_buf, sems = refs[tasks - 1 :]
    columns = outs[0].shape[1]
    block = columns // PIECES
    limit_copy = pltpu.make_async_copy(limits, limit_buf, sems.at[0])
    limit_copy.start()
    work = [(step, piece) for step in range(1, tasks) for piece in range(PIECES)]
    copies = []
    for at, (step, piece) in enumerate(work):
        source = pl.ds(pl.multiple_of(column_start(step, columns) + piece * block, LANES), block)
        target = pl.ds(piece * block, block)
        copies.append([
            pltpu.make_async_copy(scores.at[0, 0, :, source], score_buf.at[step - 1, :, target], sems.at[2 * at + 1]),
            pltpu.make_async_copy(deltas.at[0, 0, :, source], delta_buf.at[step - 1, :, target], sems.at[2 * at + 2]),
        ])
        for copy in copies[-1]:
            copy.start()
    limit_copy.wait()
    limit = limit_buf[0, 0, own_expert()]
    for at, (step, piece) in enumerate(work):
        for copy in copies[at]:
            copy.wait()
        where = pl.ds(piece * block, block)
        outs[step - 1][:, where] = mask_block(delta_buf[step - 1, :, where], score_buf[step - 1, :, where], limit)


def row_sums(changes):
    values = [change.astype(jnp.float32) for change in changes]
    values = [sum(value[at : at + 8] for at in range(8, value.shape[0], 8)) + value[:8] for value in values]
    if len(values) != 8:
        return jnp.concatenate([jnp.sum(value, axis=0, keepdims=True) for value in values], axis=0)
    lane = lax.broadcasted_iota(jnp.int32, values[0].shape, 0)
    for shift in (4, 2, 1):
        low = lane % (2 * shift) < shift
        values = [
            jnp.where(low, one + pltpu.roll(one, 8 - shift, 0), two + pltpu.roll(two, shift, 0))
            for one, two in zip(values[:shift], values[shift:])
        ]
    return values[0]


def sums_kernel(deltas, copied, packs, sems):
    tasks, folded, packed = packs.shape
    half = packed - 2 * LANES
    layers, rows, _ = copied.shape
    columns = 2 * half
    block = min(BLOCK, half)
    places = half // block
    groups = lax.axis_size("shard") // EXPERTS
    work = [(step, place) for step in range(tasks) for place in range(places)]
    copies = []
    sources = []
    for step, place in work:
        start = column_start(step, columns) + place * block
        sources.append([pl.ds(pl.multiple_of(start + part * half, LANES), block) for part in range(2)])
        copies.append([
            pltpu.make_async_copy(deltas.at[0, :, :, source], copied.at[:, :, source], sems.at[2 * len(copies) + part])
            for part, source in enumerate(sources[-1])
        ])
        for copy in copies[-1]:
            copy.start()
    totals = jnp.zeros((folded, LANES), jnp.float32)
    for at, (step, place) in enumerate(work):
        for copy in copies[at]:
            copy.wait()
        sums = row_sums([jnp.abs(copied[layer, :, source]) for source in sources[at] for layer in range(layers)])
        means = sums * (1.0 / (rows * groups))
        packs[step, :, place * block : (place + 1) * block] = means.astype(jnp.bfloat16)
        for tile in range(0, block, LANES):
            totals = totals + means[:, tile : tile + LANES]
    for step in range(tasks):
        store_split(packs.at[step], totals)


def store_split(pack, totals):
    half = pack.shape[1] - 2 * LANES
    high = totals.astype(jnp.bfloat16)
    pack[:, half : half + LANES] = high
    pack[:, half + LANES :] = (totals - high.astype(jnp.float32)).astype(jnp.bfloat16)


def mask_kernel(chunks, own_layers, limits, scores, copied, *refs):
    tasks = lax.axis_size("task")
    _, _, width = copied.shape
    columns = width // tasks
    count = len(chunks) * (tasks - 1)
    sent, refs = refs[:count], refs[count:]
    if own_layers:
        own, refs = refs[0], refs[1:]
    limit_buf, score_buf, sems = refs
    limit_copy = pltpu.make_async_copy(limits, limit_buf, sems.at[0])
    limit_copy.start()
    work = []
    for at, chunk in enumerate(chunks):
        for step in range(1, tasks):
            offset = 0
            for layer, begin, end in chunk:
                size = (end - begin) * columns // 4
                work.append((sent[at * (tasks - 1) + step - 1], offset, layer, step, begin * columns // 4, size))
                offset += size
    work += [(own.at[layer], 0, layer, 0, 0, columns) for layer in own_layers]
    copies = []
    for at, (_, _, layer, step, begin, size) in enumerate(work):
        source = pl.ds(pl.multiple_of(column_start(step, columns) + begin, LANES), size)
        copies.append(pltpu.make_async_copy(scores.at[0, layer, :, source], score_buf.at[at, :, :size], sems.at[at + 1]))
        copies[-1].start()
    limit_copy.wait()
    for at, (target, offset, layer, step, begin, size) in enumerate(work):
        start = column_start(step, columns) + begin
        limit = limit_buf[0, layer, own_expert()]
        copies[at].wait()

        def body(place, block):
            change = copied[layer, :, pl.ds(pl.multiple_of(start + place, LANES), block)]
            kept = mask_block(change, score_buf[at, :, pl.ds(place, block)], limit)
            target[:, pl.ds(pl.multiple_of(offset + place, LANES), block)] = kept

        blocks(size, body)


def slot_lanes(width):
    return pl.ds(pl.multiple_of(lax.rem(lax.axis_index("shard"), 2) * width, LANES), width)


def pair_kernel(mine, theirs, means, totals, *refs):
    packs, both_buf = refs[:-1], refs[-1]
    tasks, _, packed = mine.shape
    half = packed - 2 * LANES
    both = mine[...].astype(jnp.float32) + theirs[...].astype(jnp.float32)
    both_buf[...] = both
    means[...] = both[0, :, :half]
    total = both[0, :, half : half + LANES] + both[0, :, half + LANES :]
    totals[...] = total
    for step in range(1, tasks):
        packs[step - 1][:, : half // 2] = both_buf[step, :, slot_lanes(half // 2)].astype(jnp.bfloat16)
        store_split(packs[step - 1], total)


def join_kernel(own_means, own_totals, *refs):
    tasks = lax.axis_size("task")
    means, totals = refs[2 * tasks - 2 :]
    half = means.shape[2]
    quarter = half // 2
    means[0] = own_means[...]
    totals[0] = own_totals[...]
    other = lax.rem(lax.axis_index("shard") + 1, 2) * quarter
    for step in range(1, tasks):
        mine, theirs = refs[2 * step - 2 : 2 * step]
        means[step, :, slot_lanes(quarter)] = mine[:, :quarter].astype(jnp.float32)
        means[step, :, pl.ds(pl.multiple_of(other, LANES), quarter)] = theirs[:, :quarter].astype(jnp.float32)
        both = mine[:, quarter:].astype(jnp.float32)
        totals[step] = both[:, :LANES] + both[:, LANES:]


def scale_kernel(means, totals, scales):
    tasks, folded, _ = means.shape
    for step in range(tasks):
        total = jnp.sum(totals[step], axis=1, keepdims=True)
        total = total + jnp.concatenate([total[folded // 2 :], total[: folded // 2]], axis=0)
        grand = total * (1.0 / (EXPERTS * FF))
        mean = means[step]
        rounded = (0.2 + 0.7 * mean / (mean + grand)).astype(jnp.bfloat16)
        scales[step] = 1.0 / rounded.astype(jnp.float32)


def merge_kernel(chunks, tasks, aliased, scales, own, *refs):
    half = scales.shape[2]
    layers = own.shape[0]
    columns = 2 * half
    arrived = refs[: len(chunks) * (tasks - 1)]
    out, buf, sems = refs[len(arrived) + aliased :]
    pieces = []
    base = 0
    for place, chunk in enumerate(chunks):
        offset = 0
        for layer, begin, end in chunk:
            for part in range(2):
                low, high = [min(max(at * columns // 4 - part * half, 0), half) for at in (begin, end)]
                if high > low:
                    pieces.append((place, base, layer, part, low, high - low, offset))
                    offset += high - low
        base += offset
    copies = []
    for at, (place, base, layer, part, low, size, offset) in enumerate(pieces):
        row = part * layers + layer

        def body(shift, block):
            narrow = pl.ds(pl.multiple_of(low + shift, LANES), block)
            mine = pl.ds(pl.multiple_of(part * half + low + shift, LANES), block)
            source = pl.ds(pl.multiple_of(offset + shift, LANES), block)
            merged = own[layer, :, mine].astype(jnp.float32) * scales[0, row : row + 1, narrow]
            for step in range(1, tasks):
                other = arrived[place * (tasks - 1) + step - 1][:, source].astype(jnp.float32)
                merged = merged + other * scales[step, row : row + 1, narrow]
            buf[:, pl.ds(pl.multiple_of(base + offset + shift, LANES), block)] = merged.astype(jnp.bfloat16)

        blocks(size, body)
        copies.append(pltpu.make_async_copy(
            buf.at[:, pl.ds(base + offset, size)], out.at[layer, :, pl.ds(part * half + low, size)], sems.at[at]))
        copies[-1].start()
    for copy in copies:
        copy.wait()


def cost(flops, moved):
    return pl.CostEstimate(flops=flops, bytes_accessed=moved, transcendentals=0)


def on_chip(value):
    return pltpu.with_memory_space_constraint(value, pltpu.VMEM)


def merge_all(task_deltas, rank_scores, keep_limits):
    shards, tasks = lax.axis_size("shard"), lax.axis_size("task")
    groups = shards // EXPERTS
    group_bits = groups.bit_length() - 1
    layers, rows, width = task_deltas.shape[1:]
    columns = width // tasks
    half = columns // 2
    block = min(BLOCK, half)
    bf16, f32 = jnp.bfloat16, jnp.float32
    plan = chunk_plan(layers)
    slabs = [pltpu.VMEM((rows, chunk_width(chunk, columns)), bf16) for chunk in plan]

    task_deltas, rank_scores, keep_limits = [
        pltpu.with_memory_space_constraint(value, pltpu.HBM) for value in (task_deltas, rank_scores, keep_limits)
    ]
    first = pl.pallas_call(
        first_kernel,
        out_shape=[slabs[0]] * (tasks - 1),
        in_specs=[HBM] * 3,
        out_specs=[VMEM] * (tasks - 1),
        scratch_shapes=[
            pltpu.SMEM(keep_limits.shape, jnp.int32),
            pltpu.VMEM((tasks - 1, rows, columns), bf16),
            pltpu.VMEM((tasks - 1, rows, columns), jnp.int32),
            pltpu.SemaphoreType.DMA((2 * PIECES * (tasks - 1) + 1,)),
        ],
        compiler_params=pltpu.CompilerParams(vmem_limit_bytes=GRANT),
        cost_estimate=cost(10**6, 6 * rows * columns),
        name="first",
    )(keep_limits, task_deltas, rank_scores)
    arrived = [[shifted(first[step - 1], step) for step in range(1, tasks)]]

    pack = (2 * layers, half + 2 * LANES)
    copied, packs = pl.pallas_call(
        sums_kernel,
        out_shape=[pltpu.VMEM((layers, rows, width), bf16), pltpu.VMEM((tasks, *pack), bf16)],
        in_specs=[HBM],
        out_specs=[VMEM] * 2,
        scratch_shapes=[pltpu.SemaphoreType.DMA((2 * tasks * half // block,))],
        compiler_params=pltpu.CompilerParams(vmem_limit_bytes=GRANT),
        cost_estimate=cost(10**7, 2 * layers * rows * width),
        name="sums",
    )(task_deltas)

    def masks(places, own_layers):
        chunks = [plan[place] for place in places]
        shapes = [slabs[place] for place in places for _ in range(1, tasks)]
        shapes += [pltpu.VMEM((layers, rows, columns), bf16)] * bool(own_layers)
        pieces = sum(len(chunk) for chunk in chunks) * (tasks - 1) + len(own_layers)
        return pl.pallas_call(
            functools.partial(mask_kernel, chunks, own_layers),
            out_shape=shapes,
            in_specs=[HBM] * 2 + [VMEM],
            out_specs=[VMEM] * len(shapes),
            scratch_shapes=[
                pltpu.SMEM(keep_limits.shape, jnp.int32),
                pltpu.VMEM((pieces, rows, columns), jnp.int32),
                pltpu.SemaphoreType.DMA((pieces + 1,)),
            ],
            compiler_params=pltpu.CompilerParams(vmem_limit_bytes=GRANT),
            cost_estimate=cost(10**7, 6 * pieces * rows * columns),
            name="masks",
        )(keep_limits, rank_scores, on_chip(copied))

    for bit in range(1, group_bits):
        packs = packs.astype(f32) + swapped(packs, "shard", bit).astype(f32)
    theirs = swapped(packs, "shard", 0)
    sent = [*masks([1], [])]
    means, totals, *packs = pl.pallas_call(
        pair_kernel,
        out_shape=[pltpu.VMEM((2 * layers, half), f32), pltpu.VMEM((2 * layers, LANES), f32)]
        + [pltpu.VMEM((2 * layers, half // 2 + 2 * LANES), bf16)] * (tasks - 1),
        in_specs=[VMEM] * 2,
        out_specs=[VMEM] * (tasks + 1),
        scratch_shapes=[pltpu.VMEM((tasks, *pack), f32)],
        compiler_params=pltpu.CompilerParams(vmem_limit_bytes=GRANT),
        cost_estimate=cost(10**6, 8 * tasks * layers * half),
        name="pair",
    )(on_chip(packs), on_chip(theirs))
    arrivals = [shifted(packs[step - 1], step) for step in range(1, tasks)]
    arrived.append([shifted(sent[step - 1], step) for step in range(1, tasks)])
    sent += masks([*range(2, len(plan))], [])
    (own,) = masks([], [*range(layers)])
    pairs = []
    for arrival in arrivals:
        pairs += [arrival, swapped(arrival, "shard", 0)]
    for place in range(2, len(plan)):
        at = (place - 1) * (tasks - 1)
        arrived.append([shifted(sent[at + step - 1], step) for step in range(1, tasks)])

    means, totals = pl.pallas_call(
        join_kernel,
        out_shape=[pltpu.VMEM((tasks, 2 * layers, half), f32), pltpu.VMEM((tasks, 2 * layers, LANES), f32)],
        in_specs=[VMEM] * (2 * tasks),
        out_specs=[VMEM] * 2,
        compiler_params=pltpu.CompilerParams(vmem_limit_bytes=GRANT),
        cost_estimate=cost(10**6, 8 * tasks * layers * half),
        name="join",
    )(on_chip(means), on_chip(totals), *[on_chip(value) for value in pairs])
    for bit in range(group_bits, shards.bit_length() - 1):
        totals = totals + swapped(totals, "shard", bit)

    scales = pl.pallas_call(
        scale_kernel,
        out_shape=pltpu.VMEM((tasks, 2 * layers, half), f32),
        in_specs=[VMEM] * 2,
        out_specs=VMEM,
        compiler_params=pltpu.CompilerParams(vmem_limit_bytes=GRANT),
        cost_estimate=cost(10**6, 8 * tasks * layers * half),
        name="scale",
    )(on_chip(means), on_chip(totals))

    out = None
    for places in ([0, 1], *[[place] for place in range(2, len(plan))]):
        chunks = [plan[place] for place in places]
        pieces = [piece for place in places for piece in arrived[place]]
        extra = [] if out is None else [out]
        merged_width = sum(chunk_width(chunk, columns) for chunk in chunks)
        out = pl.pallas_call(
            functools.partial(merge_kernel, chunks, tasks, len(extra)),
            out_shape=jax.ShapeDtypeStruct((layers, rows, columns), bf16),
            in_specs=[VMEM] * (2 + len(pieces)) + [ANY] * len(extra),
            out_specs=ANY,
            scratch_shapes=[
                pltpu.VMEM((rows, merged_width), bf16),
                pltpu.SemaphoreType.DMA((2 * sum(len(chunk) for chunk in chunks),)),
            ],
            input_output_aliases={2 + len(pieces): 0} if extra else {},
            compiler_params=pltpu.CompilerParams(vmem_limit_bytes=GRANT),
            cost_estimate=cost(10**6, 6 * rows * merged_width),
            name="merge",
        )(on_chip(scales), on_chip(own), *[on_chip(piece) for piece in pieces], *extra)
    return out


def solution(mesh):
    return jax.shard_map(
        merge_all,
        mesh=mesh,
        in_specs=(
            P("task", None, "shard", None),
            P("task", None, "shard", None),
            P("task", None, None),
        ),
        out_specs=P(None, "shard", "task"),
        check_vma=False,
    )
```

```python
import functools
import math

import jax
import jax.numpy as jnp
from jax import lax
from jax.experimental import pallas as pl
from jax.experimental.pallas import tpu as pltpu
from jax.sharding import PartitionSpec as P


EXPERTS = 8
FF = 16384
LANES = 128
BLOCK = 2048
PIECES = 1
CUT = 5
GRANT = 16 * 2**20

ANY = pl.BlockSpec(memory_space=pl.ANY)
HBM = pl.BlockSpec(memory_space=pltpu.HBM)
VMEM = pl.BlockSpec(memory_space=pltpu.VMEM)


def crossed(value, axis, mask):
    return lax.ppermute(value, axis, [(source, source ^ mask) for source in range(lax.axis_size(axis))])


def swapped(value, axis, bit):
    return crossed(value, axis, 1 << bit)


def shifted(value, step):
    size = lax.axis_size("task")
    return lax.ppermute(value, "task", [(source, (source + step) % size) for source in range(size)])


def column_start(step, columns):
    tasks = lax.axis_size("task")
    return lax.rem(lax.axis_index("task") + step, tasks) * columns


def own_expert():
    return lax.axis_index("shard") // (lax.axis_size("shard") // EXPERTS)


def blocks(width, body):
    block = math.gcd(BLOCK, width)

    @pl.loop(0, width // block)
    def _(at):
        body(pl.multiple_of(at * block, block), block)


def chunk_plan(layers):
    last = layers - 1
    return [[(0, 0, 8)], [(layer, 0, 8) for layer in range(1, last)], [(last, 0, CUT)], [(last, CUT, 8)]]


def chunk_width(chunk, columns):
    return sum(end - begin for _, begin, end in chunk) * columns // 8


def mask_block(deltas, scores, limit):
    return jnp.where(scores < limit, deltas.astype(jnp.float32), 0.0).astype(jnp.bfloat16)


def first_kernel(limits, deltas, scores, *refs):
    tasks = lax.axis_size("task")
    outs = refs[: tasks - 1]
    limit_buf, delta_buf, score_buf, sems = refs[tasks - 1 :]
    columns = outs[0].shape[1]
    block = columns // PIECES
    limit_copy = pltpu.make_async_copy(limits, limit_buf, sems.at[0])
    limit_copy.start()
    work = [(step, piece) for step in range(1, tasks) for piece in range(PIECES)]
    copies = []
    for at, (step, piece) in enumerate(work):
        source = pl.ds(pl.multiple_of(column_start(step, columns) + piece * block, LANES), block)
        target = pl.ds(piece * block, block)
        copies.append([
            pltpu.make_async_copy(scores.at[0, 0, :, source], score_buf.at[step - 1, :, target], sems.at[2 * at + 1]),
            pltpu.make_async_copy(deltas.at[0, 0, :, source], delta_buf.at[step - 1, :, target], sems.at[2 * at + 2]),
        ])
        for copy in copies[-1]:
            copy.start()
    limit_copy.wait()
    limit = limit_buf[0, 0, own_expert()]
    for at, (step, piece) in enumerate(work):
        for copy in copies[at]:
            copy.wait()
        where = pl.ds(piece * block, block)
        outs[step - 1][:, where] = mask_block(delta_buf[step - 1, :, where], score_buf[step - 1, :, where], limit)


def row_sums(changes):
    values = [change.astype(jnp.float32) for change in changes]
    values = [sum(value[at : at + 8] for at in range(8, value.shape[0], 8)) + value[:8] for value in values]
    if len(values) != 8:
        return jnp.concatenate([jnp.sum(value, axis=0, keepdims=True) for value in values], axis=0)
    lane = lax.broadcasted_iota(jnp.int32, values[0].shape, 0)
    for shift in (4, 2, 1):
        low = lane % (2 * shift) < shift
        values = [
            jnp.where(low, one + pltpu.roll(one, 8 - shift, 0), two + pltpu.roll(two, shift, 0))
            for one, two in zip(values[:shift], values[shift:])
        ]
    return values[0]


def sums_kernel(deltas, copied, packs, sems):
    tasks, folded, packed = packs.shape
    half = packed - LANES
    layers, rows, _ = copied.shape
    columns = 2 * half
    block = min(BLOCK, half)
    places = half // block
    groups = lax.axis_size("shard") // EXPERTS
    work = [(step, place) for step in range(tasks) for place in range(places)]
    copies = []
    sources = []
    for step, place in work:
        start = column_start(step, columns) + place * block
        sources.append([pl.ds(pl.multiple_of(start + part * half, LANES), block) for part in range(2)])
        copies.append([
            pltpu.make_async_copy(deltas.at[0, :, :, source], copied.at[:, :, source], sems.at[2 * len(copies) + part])
            for part, source in enumerate(sources[-1])
        ])
        for copy in copies[-1]:
            copy.start()
    totals = jnp.zeros((folded, LANES), jnp.float32)
    for at, (step, place) in enumerate(work):
        for copy in copies[at]:
            copy.wait()
        sums = row_sums([jnp.abs(copied[layer, :, source]) for source in sources[at] for layer in range(layers)])
        means = sums * (1.0 / (rows * groups))
        packs[step, :, place * block : (place + 1) * block] = means
        for tile in range(0, block, LANES):
            totals = totals + means[:, tile : tile + LANES]
    for step in range(tasks):
        packs[step, :, half:] = totals


def store_split(pack, totals):
    half = pack.shape[1] - 2 * LANES
    high = totals.astype(jnp.bfloat16)
    pack[:, half : half + LANES] = high
    pack[:, half + LANES :] = (totals - high.astype(jnp.float32)).astype(jnp.bfloat16)


def mask_kernel(chunks, own_layers, limits, scores, copied, *refs):
    tasks = lax.axis_size("task")
    _, _, width = copied.shape
    columns = width // tasks
    count = len(chunks) * (tasks - 1)
    sent, refs = refs[:count], refs[count:]
    if own_layers:
        own, refs = refs[0], refs[1:]
    limit_buf, score_buf, sems = refs
    limit_copy = pltpu.make_async_copy(limits, limit_buf, sems.at[0])
    limit_copy.start()
    work = []
    for at, chunk in enumerate(chunks):
        for step in range(1, tasks):
            offset = 0
            for layer, begin, end in chunk:
                size = (end - begin) * columns // 8
                work.append((sent[at * (tasks - 1) + step - 1], offset, layer, step, begin * columns // 8, size))
                offset += size
    work += [(own.at[layer], 0, layer, 0, 0, columns) for layer in own_layers]
    copies = []
    for at, (_, _, layer, step, begin, size) in enumerate(work):
        source = pl.ds(pl.multiple_of(column_start(step, columns) + begin, LANES), size)
        copies.append(pltpu.make_async_copy(scores.at[0, layer, :, source], score_buf.at[at, :, :size], sems.at[at + 1]))
        copies[-1].start()
    limit_copy.wait()
    for at, (target, offset, layer, step, begin, size) in enumerate(work):
        start = column_start(step, columns) + begin
        limit = limit_buf[0, layer, own_expert()]
        copies[at].wait()

        def body(place, block):
            change = copied[layer, :, pl.ds(pl.multiple_of(start + place, LANES), block)]
            kept = mask_block(change, score_buf[at, :, pl.ds(place, block)], limit)
            target[:, pl.ds(pl.multiple_of(offset + place, LANES), block)] = kept

        blocks(size, body)


def slot_lanes(width):
    return pl.ds(pl.multiple_of(lax.rem(lax.axis_index("shard"), 2) * width, LANES), width)


def pair_kernel(mine, theirs, means, totals, *packs):
    tasks, _, packed = mine.shape
    half = packed - LANES
    means[...] = mine[0, :, :half] + theirs[0, :, :half]
    total = mine[0, :, half:] + theirs[0, :, half:]
    totals[...] = total
    for step in range(1, tasks):
        picked = mine[step, :, slot_lanes(half // 2)] + theirs[step, :, slot_lanes(half // 2)]
        packs[step - 1][:, : half // 2] = picked.astype(jnp.bfloat16)
        store_split(packs[step - 1], total)


def join_kernel(own_means, own_totals, *refs):
    tasks = lax.axis_size("task")
    means, totals = refs[2 * tasks - 2 :]
    half = means.shape[2]
    quarter = half // 2
    means[0] = own_means[...]
    totals[0] = own_totals[...]
    other = lax.rem(lax.axis_index("shard") + 1, 2) * quarter
    for step in range(1, tasks):
        mine, theirs = refs[2 * step - 2 : 2 * step]
        means[step, :, slot_lanes(quarter)] = mine[:, :quarter].astype(jnp.float32)
        means[step, :, pl.ds(pl.multiple_of(other, LANES), quarter)] = theirs[:, :quarter].astype(jnp.float32)
        both = mine[:, quarter:].astype(jnp.float32)
        totals[step] = both[:, :LANES] + both[:, LANES:]


def scale_kernel(means, totals, scales):
    tasks, folded, _ = means.shape
    for step in range(tasks):
        total = jnp.sum(totals[step], axis=1, keepdims=True)
        total = total + jnp.concatenate([total[folded // 2 :], total[: folded // 2]], axis=0)
        grand = total * (1.0 / (EXPERTS * FF))
        mean = means[step]
        rounded = (0.2 + 0.7 * mean / (mean + grand)).astype(jnp.bfloat16)
        scales[step] = 1.0 / rounded.astype(jnp.float32)


def merge_kernel(chunks, tasks, aliased, scales, own, *refs):
    half = scales.shape[2]
    layers = own.shape[0]
    columns = 2 * half
    arrived = refs[: len(chunks) * (tasks - 1)]
    out, buf, sems = refs[len(arrived) + aliased :]
    pieces = []
    base = 0
    for place, chunk in enumerate(chunks):
        offset = 0
        for layer, begin, end in chunk:
            for part in range(2):
                low, high = [min(max(at * columns // 8 - part * half, 0), half) for at in (begin, end)]
                if high > low:
                    pieces.append((place, base, layer, part, low, high - low, offset))
                    offset += high - low
        base += offset
    copies = []
    for at, (place, base, layer, part, low, size, offset) in enumerate(pieces):
        row = part * layers + layer

        def body(shift, block):
            narrow = pl.ds(pl.multiple_of(low + shift, LANES), block)
            mine = pl.ds(pl.multiple_of(part * half + low + shift, LANES), block)
            source = pl.ds(pl.multiple_of(offset + shift, LANES), block)
            merged = own[layer, :, mine].astype(jnp.float32) * scales[0, row : row + 1, narrow]
            for step in range(1, tasks):
                other = arrived[place * (tasks - 1) + step - 1][:, source].astype(jnp.float32)
                merged = merged + other * scales[step, row : row + 1, narrow]
            buf[:, pl.ds(pl.multiple_of(base + offset + shift, LANES), block)] = merged.astype(jnp.bfloat16)

        blocks(size, body)
        copies.append(pltpu.make_async_copy(
            buf.at[:, pl.ds(base + offset, size)], out.at[layer, :, pl.ds(part * half + low, size)], sems.at[at]))
        copies[-1].start()
    for copy in copies:
        copy.wait()


def cost(flops, moved):
    return pl.CostEstimate(flops=flops, bytes_accessed=moved, transcendentals=0)


def on_chip(value):
    return pltpu.with_memory_space_constraint(value, pltpu.VMEM)


def merge_all(task_deltas, rank_scores, keep_limits):
    shards, tasks = lax.axis_size("shard"), lax.axis_size("task")
    groups = shards // EXPERTS
    group_bits = groups.bit_length() - 1
    layers, rows, width = task_deltas.shape[1:]
    columns = width // tasks
    half = columns // 2
    block = min(BLOCK, half)
    bf16, f32 = jnp.bfloat16, jnp.float32
    plan = chunk_plan(layers)
    slabs = [pltpu.VMEM((rows, chunk_width(chunk, columns)), bf16) for chunk in plan]

    task_deltas, rank_scores, keep_limits = [
        pltpu.with_memory_space_constraint(value, pltpu.HBM) for value in (task_deltas, rank_scores, keep_limits)
    ]
    first = pl.pallas_call(
        first_kernel,
        out_shape=[slabs[0]] * (tasks - 1),
        in_specs=[HBM] * 3,
        out_specs=[VMEM] * (tasks - 1),
        scratch_shapes=[
            pltpu.SMEM(keep_limits.shape, jnp.int32),
            pltpu.VMEM((tasks - 1, rows, columns), bf16),
            pltpu.VMEM((tasks - 1, rows, columns), jnp.int32),
            pltpu.SemaphoreType.DMA((2 * PIECES * (tasks - 1) + 1,)),
        ],
        compiler_params=pltpu.CompilerParams(vmem_limit_bytes=GRANT),
        cost_estimate=cost(10**6, 6 * rows * columns),
        name="first",
    )(keep_limits, task_deltas, rank_scores)
    arrived = [[shifted(first[step - 1], step) for step in range(1, tasks)]]

    pack = (tasks, 2 * layers, half + LANES)
    copied, packs = pl.pallas_call(
        sums_kernel,
        out_shape=[pltpu.VMEM((layers, rows, width), bf16), pltpu.VMEM(pack, f32)],
        in_specs=[HBM],
        out_specs=[VMEM] * 2,
        scratch_shapes=[pltpu.SemaphoreType.DMA((2 * tasks * half // block,))],
        compiler_params=pltpu.CompilerParams(vmem_limit_bytes=GRANT),
        cost_estimate=cost(10**7, 2 * layers * rows * width),
        name="sums",
    )(task_deltas)

    def masks(places, own_layers):
        chunks = [plan[place] for place in places]
        shapes = [slabs[place] for place in places for _ in range(1, tasks)]
        shapes += [pltpu.VMEM((layers, rows, columns), bf16)] * bool(own_layers)
        pieces = sum(len(chunk) for chunk in chunks) * (tasks - 1) + len(own_layers)
        return pl.pallas_call(
            functools.partial(mask_kernel, chunks, own_layers),
            out_shape=shapes,
            in_specs=[HBM] * 2 + [VMEM],
            out_specs=[VMEM] * len(shapes),
            scratch_shapes=[
                pltpu.SMEM(keep_limits.shape, jnp.int32),
                pltpu.VMEM((pieces, rows, columns), jnp.int32),
                pltpu.SemaphoreType.DMA((pieces + 1,)),
            ],
            compiler_params=pltpu.CompilerParams(vmem_limit_bytes=GRANT),
            cost_estimate=cost(10**7, 6 * pieces * rows * columns),
            name="masks",
        )(keep_limits, rank_scores, on_chip(copied))

    for bit in range(1, group_bits):
        packs = packs + swapped(packs, "shard", bit)
    theirs = swapped(packs, "shard", 0)
    sent = [*masks([1], [])]
    means, totals, *packs = pl.pallas_call(
        pair_kernel,
        out_shape=[pltpu.VMEM((2 * layers, half), f32), pltpu.VMEM((2 * layers, LANES), f32)]
        + [pltpu.VMEM((2 * layers, half // 2 + 2 * LANES), bf16)] * (tasks - 1),
        in_specs=[VMEM] * 2,
        out_specs=[VMEM] * (tasks + 1),
        compiler_params=pltpu.CompilerParams(vmem_limit_bytes=GRANT),
        cost_estimate=cost(10**6, 8 * tasks * layers * half),
        name="pair",
    )(on_chip(packs), on_chip(theirs))
    arrivals = [shifted(packs[step - 1], step) for step in range(1, tasks)]
    arrived.append([shifted(sent[step - 1], step) for step in range(1, tasks)])
    sent += masks([*range(2, len(plan))], [])
    (own,) = masks([], [*range(layers)])
    pairs = []
    for arrival in arrivals:
        pairs += [arrival, swapped(arrival, "shard", 0)]
    for place in range(2, len(plan)):
        at = (place - 1) * (tasks - 1)
        arrived.append([shifted(sent[at + step - 1], step) for step in range(1, tasks)])

    means, totals = pl.pallas_call(
        join_kernel,
        out_shape=[pltpu.VMEM((tasks, 2 * layers, half), f32), pltpu.VMEM((tasks, 2 * layers, LANES), f32)],
        in_specs=[VMEM] * (2 * tasks),
        out_specs=[VMEM] * 2,
        compiler_params=pltpu.CompilerParams(vmem_limit_bytes=GRANT),
        cost_estimate=cost(10**6, 8 * tasks * layers * half),
        name="join",
    )(on_chip(means), on_chip(totals), *[on_chip(value) for value in pairs])
    for bit in range(group_bits, shards.bit_length() - 1):
        totals = totals + swapped(totals, "shard", bit)

    scales = pl.pallas_call(
        scale_kernel,
        out_shape=pltpu.VMEM((tasks, 2 * layers, half), f32),
        in_specs=[VMEM] * 2,
        out_specs=VMEM,
        compiler_params=pltpu.CompilerParams(vmem_limit_bytes=GRANT),
        cost_estimate=cost(10**6, 8 * tasks * layers * half),
        name="scale",
    )(on_chip(means), on_chip(totals))

    out = None
    for places in ([0, 1], *[[place] for place in range(2, len(plan))]):
        chunks = [plan[place] for place in places]
        pieces = [piece for place in places for piece in arrived[place]]
        extra = [] if out is None else [out]
        merged_width = sum(chunk_width(chunk, columns) for chunk in chunks)
        out = pl.pallas_call(
            functools.partial(merge_kernel, chunks, tasks, len(extra)),
            out_shape=jax.ShapeDtypeStruct((layers, rows, columns), bf16),
            in_specs=[VMEM] * (2 + len(pieces)) + [ANY] * len(extra),
            out_specs=ANY,
            scratch_shapes=[
                pltpu.VMEM((rows, merged_width), bf16),
                pltpu.SemaphoreType.DMA((2 * sum(len(chunk) for chunk in chunks),)),
            ],
            input_output_aliases={2 + len(pieces): 0} if extra else {},
            compiler_params=pltpu.CompilerParams(vmem_limit_bytes=GRANT),
            cost_estimate=cost(10**6, 6 * rows * merged_width),
            name="merge",
        )(on_chip(scales), on_chip(own), *[on_chip(piece) for piece in pieces], *extra)
    return out


def solution(mesh):
    return jax.shard_map(
        merge_all,
        mesh=mesh,
        in_specs=(
            P("task", None, "shard", None),
            P("task", None, "shard", None),
            P("task", None, None),
        ),
        out_specs=P(None, "shard", "task"),
        check_vma=False,
    )
```

```python
import functools
import math

import jax
import jax.numpy as jnp
from jax import lax
from jax.experimental import pallas as pl
from jax.experimental.pallas import tpu as pltpu
from jax.sharding import PartitionSpec as P


EXPERTS = 8
FF = 16384
LANES = 128
BLOCK = 2048
PIECES = 1
CUT = 5
GRANT = 16 * 2**20

ANY = pl.BlockSpec(memory_space=pl.ANY)
HBM = pl.BlockSpec(memory_space=pltpu.HBM)
VMEM = pl.BlockSpec(memory_space=pltpu.VMEM)


def crossed(value, axis, mask):
    return lax.ppermute(value, axis, [(source, source ^ mask) for source in range(lax.axis_size(axis))])


def swapped(value, axis, bit):
    return crossed(value, axis, 1 << bit)


def shifted(value, step):
    size = lax.axis_size("task")
    return lax.ppermute(value, "task", [(source, (source + step) % size) for source in range(size)])


def shifted_across(value, step):
    tasks = lax.axis_size("task")
    pairs = [
        (shard * tasks + source, (shard ^ 1) * tasks + (source + step) % tasks)
        for shard in range(lax.axis_size("shard"))
        for source in range(tasks)
    ]
    return lax.ppermute(value, ("shard", "task"), pairs)


def column_start(step, columns):
    tasks = lax.axis_size("task")
    return lax.rem(lax.axis_index("task") + step, tasks) * columns


def own_expert():
    return lax.axis_index("shard") // (lax.axis_size("shard") // EXPERTS)


def blocks(width, body):
    block = math.gcd(BLOCK, width)

    @pl.loop(0, width // block)
    def _(at):
        body(pl.multiple_of(at * block, block), block)


def chunk_plan(layers):
    last = layers - 1
    return [[(0, 0, 8)], [(layer, 0, 8) for layer in range(1, last)], [(last, 0, CUT)], [(last, CUT, 8)]]


def chunk_width(chunk, columns):
    return sum(end - begin for _, begin, end in chunk) * columns // 8


def mask_block(deltas, scores, limit):
    return jnp.where(scores < limit, deltas.astype(jnp.float32), 0.0).astype(jnp.bfloat16)


def first_kernel(limits, deltas, scores, *refs):
    tasks = lax.axis_size("task")
    outs = refs[: tasks - 1]
    limit_buf, delta_buf, score_buf, sems = refs[tasks - 1 :]
    columns = outs[0].shape[1]
    block = columns // PIECES
    limit_copy = pltpu.make_async_copy(limits, limit_buf, sems.at[0])
    limit_copy.start()
    work = [(step, piece) for step in range(1, tasks) for piece in range(PIECES)]
    copies = []
    for at, (step, piece) in enumerate(work):
        source = pl.ds(pl.multiple_of(column_start(step, columns) + piece * block, LANES), block)
        target = pl.ds(piece * block, block)
        copies.append([
            pltpu.make_async_copy(scores.at[0, 0, :, source], score_buf.at[step - 1, :, target], sems.at[2 * at + 1]),
            pltpu.make_async_copy(deltas.at[0, 0, :, source], delta_buf.at[step - 1, :, target], sems.at[2 * at + 2]),
        ])
        for copy in copies[-1]:
            copy.start()
    limit_copy.wait()
    limit = limit_buf[0, 0, own_expert()]
    for at, (step, piece) in enumerate(work):
        for copy in copies[at]:
            copy.wait()
        where = pl.ds(piece * block, block)
        outs[step - 1][:, where] = mask_block(delta_buf[step - 1, :, where], score_buf[step - 1, :, where], limit)


def row_sums(changes):
    values = [change.astype(jnp.float32) for change in changes]
    values = [sum(value[at : at + 8] for at in range(8, value.shape[0], 8)) + value[:8] for value in values]
    if len(values) != 8:
        return jnp.concatenate([jnp.sum(value, axis=0, keepdims=True) for value in values], axis=0)
    lane = lax.broadcasted_iota(jnp.int32, values[0].shape, 0)
    for shift in (4, 2, 1):
        low = lane % (2 * shift) < shift
        values = [
            jnp.where(low, one + pltpu.roll(one, 8 - shift, 0), two + pltpu.roll(two, shift, 0))
            for one, two in zip(values[:shift], values[shift:])
        ]
    return values[0]


def sums_kernel(deltas, copied, packs, sems):
    tasks, folded, packed = packs.shape
    half = packed - LANES
    layers, rows, _ = copied.shape
    columns = 2 * half
    block = min(BLOCK, half)
    places = half // block
    groups = lax.axis_size("shard") // EXPERTS
    work = [(step, place) for step in range(tasks) for place in range(places)]
    copies = []
    sources = []
    for step, place in work:
        start = column_start(step, columns) + place * block
        sources.append([pl.ds(pl.multiple_of(start + part * half, LANES), block) for part in range(2)])
        copies.append([
            pltpu.make_async_copy(deltas.at[0, :, :, source], copied.at[:, :, source], sems.at[2 * len(copies) + part])
            for part, source in enumerate(sources[-1])
        ])
        for copy in copies[-1]:
            copy.start()
    totals = jnp.zeros((folded, LANES), jnp.float32)
    for at, (step, place) in enumerate(work):
        for copy in copies[at]:
            copy.wait()
        sums = row_sums([jnp.abs(copied[layer, :, source]) for source in sources[at] for layer in range(layers)])
        means = sums * (1.0 / (rows * groups))
        packs[step, :, place * block : (place + 1) * block] = means
        for tile in range(0, block, LANES):
            totals = totals + means[:, tile : tile + LANES]
    for step in range(tasks):
        packs[step, :, half:] = totals


def store_split(pack, totals):
    half = pack.shape[1] - 2 * LANES
    high = totals.astype(jnp.bfloat16)
    pack[:, half : half + LANES] = high
    pack[:, half + LANES :] = (totals - high.astype(jnp.float32)).astype(jnp.bfloat16)


def mask_kernel(chunks, own_layers, limits, scores, copied, *refs):
    tasks = lax.axis_size("task")
    _, _, width = copied.shape
    columns = width // tasks
    count = len(chunks) * (tasks - 1)
    sent, refs = refs[:count], refs[count:]
    if own_layers:
        own, refs = refs[0], refs[1:]
    limit_buf, score_buf, sems = refs
    limit_copy = pltpu.make_async_copy(limits, limit_buf, sems.at[0])
    limit_copy.start()
    work = []
    for at, chunk in enumerate(chunks):
        for step in range(1, tasks):
            offset = 0
            for layer, begin, end in chunk:
                size = (end - begin) * columns // 8
                work.append((sent[at * (tasks - 1) + step - 1], offset, layer, step, begin * columns // 8, size))
                offset += size
    work += [(own.at[layer], 0, layer, 0, 0, columns) for layer in own_layers]
    copies = []
    for at, (_, _, layer, step, begin, size) in enumerate(work):
        source = pl.ds(pl.multiple_of(column_start(step, columns) + begin, LANES), size)
        copies.append(pltpu.make_async_copy(scores.at[0, layer, :, source], score_buf.at[at, :, :size], sems.at[at + 1]))
        copies[-1].start()
    limit_copy.wait()
    for at, (target, offset, layer, step, begin, size) in enumerate(work):
        start = column_start(step, columns) + begin
        limit = limit_buf[0, layer, own_expert()]
        copies[at].wait()

        def body(place, block):
            change = copied[layer, :, pl.ds(pl.multiple_of(start + place, LANES), block)]
            kept = mask_block(change, score_buf[at, :, pl.ds(place, block)], limit)
            target[:, pl.ds(pl.multiple_of(offset + place, LANES), block)] = kept

        blocks(size, body)


def slot_lanes(width):
    return pl.ds(pl.multiple_of(lax.rem(lax.axis_index("shard"), 2) * width, LANES), width)


def pair_kernel(mine, theirs, means, totals, *packs):
    tasks, _, packed = mine.shape
    half = packed - LANES
    means[...] = mine[0, :, :half] + theirs[0, :, :half]
    total = mine[0, :, half:] + theirs[0, :, half:]
    totals[...] = total
    for step in range(1, tasks):
        picked = mine[step, :, slot_lanes(half // 2)] + theirs[step, :, slot_lanes(half // 2)]
        packs[step - 1][:, : half // 2] = picked.astype(jnp.bfloat16)
        store_split(packs[step - 1], total)


def join_kernel(own_means, own_totals, *refs):
    tasks = lax.axis_size("task")
    means, totals = refs[2 * tasks - 2 :]
    half = means.shape[2]
    quarter = half // 2
    means[0] = own_means[...]
    totals[0] = own_totals[...]
    other = lax.rem(lax.axis_index("shard") + 1, 2) * quarter
    for step in range(1, tasks):
        mine, theirs = refs[2 * step - 2 : 2 * step]
        means[step, :, slot_lanes(quarter)] = mine[:, :quarter].astype(jnp.float32)
        means[step, :, pl.ds(pl.multiple_of(other, LANES), quarter)] = theirs[:, :quarter].astype(jnp.float32)
        both = mine[:, quarter:].astype(jnp.float32)
        totals[step] = both[:, :LANES] + both[:, LANES:]


def scale_kernel(means, totals, scales):
    tasks, folded, _ = means.shape
    for step in range(tasks):
        total = jnp.sum(totals[step], axis=1, keepdims=True)
        total = total + jnp.concatenate([total[folded // 2 :], total[: folded // 2]], axis=0)
        grand = total * (1.0 / (EXPERTS * FF))
        mean = means[step]
        rounded = (0.2 + 0.7 * mean / (mean + grand)).astype(jnp.bfloat16)
        scales[step] = 1.0 / rounded.astype(jnp.float32)


def merge_kernel(chunks, tasks, aliased, scales, own, *refs):
    half = scales.shape[2]
    layers = own.shape[0]
    columns = 2 * half
    arrived = refs[: len(chunks) * (tasks - 1)]
    out, buf, sems = refs[len(arrived) + aliased :]
    pieces = []
    base = 0
    for place, chunk in enumerate(chunks):
        offset = 0
        for layer, begin, end in chunk:
            for part in range(2):
                low, high = [min(max(at * columns // 8 - part * half, 0), half) for at in (begin, end)]
                if high > low:
                    pieces.append((place, base, layer, part, low, high - low, offset))
                    offset += high - low
        base += offset
    copies = []
    for at, (place, base, layer, part, low, size, offset) in enumerate(pieces):
        row = part * layers + layer

        def body(shift, block):
            narrow = pl.ds(pl.multiple_of(low + shift, LANES), block)
            mine = pl.ds(pl.multiple_of(part * half + low + shift, LANES), block)
            source = pl.ds(pl.multiple_of(offset + shift, LANES), block)
            merged = own[layer, :, mine].astype(jnp.float32) * scales[0, row : row + 1, narrow]
            for step in range(1, tasks):
                other = arrived[place * (tasks - 1) + step - 1][:, source].astype(jnp.float32)
                merged = merged + other * scales[step, row : row + 1, narrow]
            buf[:, pl.ds(pl.multiple_of(base + offset + shift, LANES), block)] = merged.astype(jnp.bfloat16)

        blocks(size, body)
        copies.append(pltpu.make_async_copy(
            buf.at[:, pl.ds(base + offset, size)], out.at[layer, :, pl.ds(part * half + low, size)], sems.at[at]))
        copies[-1].start()
    for copy in copies:
        copy.wait()


def cost(flops, moved):
    return pl.CostEstimate(flops=flops, bytes_accessed=moved, transcendentals=0)


def on_chip(value):
    return pltpu.with_memory_space_constraint(value, pltpu.VMEM)


def merge_all(task_deltas, rank_scores, keep_limits):
    shards, tasks = lax.axis_size("shard"), lax.axis_size("task")
    groups = shards // EXPERTS
    group_bits = groups.bit_length() - 1
    layers, rows, width = task_deltas.shape[1:]
    columns = width // tasks
    half = columns // 2
    block = min(BLOCK, half)
    bf16, f32 = jnp.bfloat16, jnp.float32
    plan = chunk_plan(layers)
    slabs = [pltpu.VMEM((rows, chunk_width(chunk, columns)), bf16) for chunk in plan]

    task_deltas, rank_scores, keep_limits = [
        pltpu.with_memory_space_constraint(value, pltpu.HBM) for value in (task_deltas, rank_scores, keep_limits)
    ]
    first = pl.pallas_call(
        first_kernel,
        out_shape=[slabs[0]] * (tasks - 1),
        in_specs=[HBM] * 3,
        out_specs=[VMEM] * (tasks - 1),
        scratch_shapes=[
            pltpu.SMEM(keep_limits.shape, jnp.int32),
            pltpu.VMEM((tasks - 1, rows, columns), bf16),
            pltpu.VMEM((tasks - 1, rows, columns), jnp.int32),
            pltpu.SemaphoreType.DMA((2 * PIECES * (tasks - 1) + 1,)),
        ],
        compiler_params=pltpu.CompilerParams(vmem_limit_bytes=GRANT),
        cost_estimate=cost(10**6, 6 * rows * columns),
        name="first",
    )(keep_limits, task_deltas, rank_scores)
    arrived = [[shifted(first[step - 1], step) for step in range(1, tasks)]]

    pack = (tasks, 2 * layers, half + LANES)
    copied, packs = pl.pallas_call(
        sums_kernel,
        out_shape=[pltpu.VMEM((layers, rows, width), bf16), pltpu.VMEM(pack, f32)],
        in_specs=[HBM],
        out_specs=[VMEM] * 2,
        scratch_shapes=[pltpu.SemaphoreType.DMA((2 * tasks * half // block,))],
        compiler_params=pltpu.CompilerParams(vmem_limit_bytes=GRANT),
        cost_estimate=cost(10**7, 2 * layers * rows * width),
        name="sums",
    )(task_deltas)

    def masks(places, own_layers):
        chunks = [plan[place] for place in places]
        shapes = [slabs[place] for place in places for _ in range(1, tasks)]
        shapes += [pltpu.VMEM((layers, rows, columns), bf16)] * bool(own_layers)
        pieces = sum(len(chunk) for chunk in chunks) * (tasks - 1) + len(own_layers)
        return pl.pallas_call(
            functools.partial(mask_kernel, chunks, own_layers),
            out_shape=shapes,
            in_specs=[HBM] * 2 + [VMEM],
            out_specs=[VMEM] * len(shapes),
            scratch_shapes=[
                pltpu.SMEM(keep_limits.shape, jnp.int32),
                pltpu.VMEM((pieces, rows, columns), jnp.int32),
                pltpu.SemaphoreType.DMA((pieces + 1,)),
            ],
            compiler_params=pltpu.CompilerParams(vmem_limit_bytes=GRANT),
            cost_estimate=cost(10**7, 6 * pieces * rows * columns),
            name="masks",
        )(keep_limits, rank_scores, on_chip(copied))

    for bit in range(1, group_bits):
        packs = packs + swapped(packs, "shard", bit)
    theirs = swapped(packs, "shard", 0)
    sent = [*masks([1], [])]
    means, totals, *packs = pl.pallas_call(
        pair_kernel,
        out_shape=[pltpu.VMEM((2 * layers, half), f32), pltpu.VMEM((2 * layers, LANES), f32)]
        + [pltpu.VMEM((2 * layers, half // 2 + 2 * LANES), bf16)] * (tasks - 1),
        in_specs=[VMEM] * 2,
        out_specs=[VMEM] * (tasks + 1),
        compiler_params=pltpu.CompilerParams(vmem_limit_bytes=GRANT),
        cost_estimate=cost(10**6, 8 * tasks * layers * half),
        name="pair",
    )(on_chip(packs), on_chip(theirs))
    arrivals = [shifted(packs[step - 1], step) for step in range(1, tasks)]
    arrived.append([shifted(sent[step - 1], step) for step in range(1, tasks)])
    sent += masks([*range(2, len(plan))], [])
    (own,) = masks([], [*range(layers)])
    pairs = []
    for arrival in arrivals:
        pairs += [arrival, swapped(arrival, "shard", 0)]
    last = len(plan) - 1
    for place in range(2, last):
        at = (place - 1) * (tasks - 1)
        arrived.append([shifted(sent[at + step - 1], step) for step in range(1, tasks)])
    exchanged = [swapped(sent[(last - 1) * (tasks - 1) + step - 1], "shard", 0) for step in range(1, tasks)]
    arrived.append([shifted_across(exchanged[step - 1], step) for step in range(1, tasks)])

    means, totals = pl.pallas_call(
        join_kernel,
        out_shape=[pltpu.VMEM((tasks, 2 * layers, half), f32), pltpu.VMEM((tasks, 2 * layers, LANES), f32)],
        in_specs=[VMEM] * (2 * tasks),
        out_specs=[VMEM] * 2,
        compiler_params=pltpu.CompilerParams(vmem_limit_bytes=GRANT),
        cost_estimate=cost(10**6, 8 * tasks * layers * half),
        name="join",
    )(on_chip(means), on_chip(totals), *[on_chip(value) for value in pairs])
    for bit in range(group_bits, shards.bit_length() - 1):
        totals = totals + swapped(totals, "shard", bit)

    scales = pl.pallas_call(
        scale_kernel,
        out_shape=pltpu.VMEM((tasks, 2 * layers, half), f32),
        in_specs=[VMEM] * 2,
        out_specs=VMEM,
        compiler_params=pltpu.CompilerParams(vmem_limit_bytes=GRANT),
        cost_estimate=cost(10**6, 8 * tasks * layers * half),
        name="scale",
    )(on_chip(means), on_chip(totals))

    out = None
    for places in ([0, 1], *[[place] for place in range(2, len(plan))]):
        chunks = [plan[place] for place in places]
        pieces = [piece for place in places for piece in arrived[place]]
        extra = [] if out is None else [out]
        merged_width = sum(chunk_width(chunk, columns) for chunk in chunks)
        out = pl.pallas_call(
            functools.partial(merge_kernel, chunks, tasks, len(extra)),
            out_shape=jax.ShapeDtypeStruct((layers, rows, columns), bf16),
            in_specs=[VMEM] * (2 + len(pieces)) + [ANY] * len(extra),
            out_specs=ANY,
            scratch_shapes=[
                pltpu.VMEM((rows, merged_width), bf16),
                pltpu.SemaphoreType.DMA((2 * sum(len(chunk) for chunk in chunks),)),
            ],
            input_output_aliases={2 + len(pieces): 0} if extra else {},
            compiler_params=pltpu.CompilerParams(vmem_limit_bytes=GRANT),
            cost_estimate=cost(10**6, 6 * rows * merged_width),
            name="merge",
        )(on_chip(scales), on_chip(own), *[on_chip(piece) for piece in pieces], *extra)
    return out


def solution(mesh):
    return jax.shard_map(
        merge_all,
        mesh=mesh,
        in_specs=(
            P("task", None, "shard", None),
            P("task", None, "shard", None),
            P("task", None, None),
        ),
        out_specs=P(None, "shard", "task"),
        check_vma=False,
    )
```

```python
import functools
import math

import jax
import jax.numpy as jnp
from jax import lax
from jax.experimental import pallas as pl
from jax.experimental.pallas import tpu as pltpu
from jax.sharding import PartitionSpec as P


EXPERTS = 8
FF = 16384
LANES = 128
BLOCK = 2048
CUT = 4
EXTRA = 0
GRANT = 16 * 2**20

ANY = pl.BlockSpec(memory_space=pl.ANY)
HBM = pl.BlockSpec(memory_space=pltpu.HBM)
VMEM = pl.BlockSpec(memory_space=pltpu.VMEM)


def crossed(value, axis, mask):
    return lax.ppermute(value, axis, [(source, source ^ mask) for source in range(lax.axis_size(axis))])


def swapped(value, axis, bit):
    return crossed(value, axis, 1 << bit)


def shifted(value, step):
    size = lax.axis_size("task")
    return lax.ppermute(value, "task", [(source, (source + step) % size) for source in range(size)])


def shifted_across(value, step):
    tasks = lax.axis_size("task")
    pairs = [
        (shard * tasks + source, (shard ^ 1) * tasks + (source + step) % tasks)
        for shard in range(lax.axis_size("shard"))
        for source in range(tasks)
    ]
    return lax.ppermute(value, ("shard", "task"), pairs)


def column_start(step, columns):
    tasks = lax.axis_size("task")
    return lax.rem(lax.axis_index("task") + step, tasks) * columns


def own_expert():
    return lax.axis_index("shard") // (lax.axis_size("shard") // EXPERTS)


def blocks(width, body):
    block = width if width <= 2 * BLOCK else math.gcd(BLOCK, width)
    if block == width:
        body(0, block)
        return

    @pl.loop(0, width // block)
    def _(at):
        body(pl.multiple_of(at * block, block), block)


def chunk_plan(layers):
    last = layers - 1
    middle = [(1, EXTRA, 8), *[(layer, 0, 8) for layer in range(2, last)]]
    return [[(0, 0, 8)], middle, [(last, 0, CUT)], [(last, CUT, 8)]]


def chunk_width(chunk, columns):
    return sum(end - begin for _, begin, end in chunk) * columns // 8


def mask_block(deltas, scores, limit):
    return jnp.where(scores < limit, deltas.astype(jnp.float32), 0.0).astype(jnp.bfloat16)


def first_kernel(chunk, limits, deltas, scores, *refs):
    tasks = lax.axis_size("task")
    outs = refs[: tasks - 1]
    limit_buf, delta_buf, score_buf, sems = refs[tasks - 1 :]
    columns = deltas.shape[3] // tasks
    limit_copy = pltpu.make_async_copy(limits, limit_buf, sems.at[0])
    limit_copy.start()
    work = []
    for step in range(1, tasks):
        offset = 0
        for layer, begin, end in chunk:
            size = (end - begin) * columns // 8
            source = pl.ds(pl.multiple_of(column_start(step, columns) + begin * columns // 8, LANES), size)
            target = pl.ds(offset, size)
            at = 2 * len(work)
            copies = [
                pltpu.make_async_copy(scores.at[0, layer, :, source], score_buf.at[step - 1, :, target], sems.at[at + 1]),
                pltpu.make_async_copy(deltas.at[0, layer, :, source], delta_buf.at[step - 1, :, target], sems.at[at + 2]),
            ]
            for copy in copies:
                copy.start()
            work.append((step, layer, target, copies))
            offset += size
    limit_copy.wait()
    for step, layer, target, copies in work:
        for copy in copies:
            copy.wait()
        limit = limit_buf[0, layer, own_expert()]
        outs[step - 1][:, target] = mask_block(delta_buf[step - 1, :, target], score_buf[step - 1, :, target], limit)


def row_sums(changes):
    values = [change.astype(jnp.float32) for change in changes]
    values = [sum(value[at : at + 8] for at in range(8, value.shape[0], 8)) + value[:8] for value in values]
    if len(values) != 8:
        return jnp.concatenate([jnp.sum(value, axis=0, keepdims=True) for value in values], axis=0)
    lane = lax.broadcasted_iota(jnp.int32, values[0].shape, 0)
    for shift in (4, 2, 1):
        low = lane % (2 * shift) < shift
        values = [
            jnp.where(low, one + pltpu.roll(one, 8 - shift, 0), two + pltpu.roll(two, shift, 0))
            for one, two in zip(values[:shift], values[shift:])
        ]
    return values[0]


def sums_kernel(deltas, copied, packs, sems):
    tasks, folded, packed = packs.shape
    half = packed - LANES
    layers, rows, _ = copied.shape
    columns = 2 * half
    block = min(BLOCK, half)
    places = half // block
    groups = lax.axis_size("shard") // EXPERTS
    work = [(step, place) for step in range(tasks) for place in range(places)]
    copies = []
    sources = []
    for step, place in work:
        start = column_start(step, columns) + place * block
        sources.append([pl.ds(pl.multiple_of(start + part * half, LANES), block) for part in range(2)])
        copies.append([
            pltpu.make_async_copy(deltas.at[0, :, :, source], copied.at[:, :, source], sems.at[2 * len(copies) + part])
            for part, source in enumerate(sources[-1])
        ])
        for copy in copies[-1]:
            copy.start()
    totals = jnp.zeros((folded, LANES), jnp.float32)
    for at, (step, place) in enumerate(work):
        for copy in copies[at]:
            copy.wait()
        sums = row_sums([jnp.abs(copied[layer, :, source]) for source in sources[at] for layer in range(layers)])
        means = sums * (1.0 / (rows * groups))
        packs[step, :, place * block : (place + 1) * block] = means
        for tile in range(0, block, LANES):
            totals = totals + means[:, tile : tile + LANES]
    for step in range(tasks):
        packs[step, :, half:] = totals


def store_split(pack, totals):
    half = pack.shape[1] - 2 * LANES
    high = totals.astype(jnp.bfloat16)
    pack[:, half : half + LANES] = high
    pack[:, half + LANES :] = (totals - high.astype(jnp.float32)).astype(jnp.bfloat16)


def mask_kernel(chunks, own_layers, limits, scores, copied, *refs):
    tasks = lax.axis_size("task")
    _, _, width = copied.shape
    columns = width // tasks
    count = len(chunks) * (tasks - 1)
    sent, refs = refs[:count], refs[count:]
    if own_layers:
        own, refs = refs[0], refs[1:]
    limit_buf, score_buf, sems = refs
    limit_copy = pltpu.make_async_copy(limits, limit_buf, sems.at[0])
    limit_copy.start()
    work = []
    for at, chunk in enumerate(chunks):
        for step in range(1, tasks):
            offset = 0
            for layer, begin, end in chunk:
                size = (end - begin) * columns // 8
                work.append((sent[at * (tasks - 1) + step - 1], offset, layer, step, begin * columns // 8, size))
                offset += size
    work += [(own.at[layer], 0, layer, 0, 0, columns) for layer in own_layers]
    copies = []
    for at, (_, _, layer, step, begin, size) in enumerate(work):
        source = pl.ds(pl.multiple_of(column_start(step, columns) + begin, LANES), size)
        copies.append(pltpu.make_async_copy(scores.at[0, layer, :, source], score_buf.at[at, :, :size], sems.at[at + 1]))
        copies[-1].start()
    limit_copy.wait()
    for at, (target, offset, layer, step, begin, size) in enumerate(work):
        start = column_start(step, columns) + begin
        limit = limit_buf[0, layer, own_expert()]
        copies[at].wait()

        def body(place, block):
            change = copied[layer, :, pl.ds(pl.multiple_of(start + place, LANES), block)]
            kept = mask_block(change, score_buf[at, :, pl.ds(place, block)], limit)
            target[:, pl.ds(pl.multiple_of(offset + place, LANES), block)] = kept

        blocks(size, body)


def slot_lanes(width):
    return pl.ds(pl.multiple_of(lax.rem(lax.axis_index("shard"), 2) * width, LANES), width)


def pair_kernel(mine, theirs, means, totals, *packs):
    tasks, _, packed = mine.shape
    half = packed - LANES
    means[...] = mine[0, :, :half] + theirs[0, :, :half]
    total = mine[0, :, half:] + theirs[0, :, half:]
    totals[...] = total
    for step in range(1, tasks):
        picked = mine[step, :, slot_lanes(half // 2)] + theirs[step, :, slot_lanes(half // 2)]
        packs[step - 1][:, : half // 2] = picked.astype(jnp.bfloat16)
        store_split(packs[step - 1], total)


def unpack_kernel(own_totals, *refs):
    arrivals, totals = refs[:-1], refs[-1]
    totals[0] = own_totals[...]
    for step, arrival in enumerate(arrivals, 1):
        both = arrival[:, arrival.shape[1] - 2 * LANES :].astype(jnp.float32)
        totals[step] = both[:, :LANES] + both[:, LANES:]


def join_kernel(own_means, *refs):
    pairs, means = refs[:-1], refs[-1]
    quarter = means.shape[2] // 2
    means[0] = own_means[...]
    other = lax.rem(lax.axis_index("shard") + 1, 2) * quarter
    for step in range(1, means.shape[0]):
        mine, theirs = pairs[2 * step - 2 : 2 * step]
        means[step, :, slot_lanes(quarter)] = mine[:, :quarter].astype(jnp.float32)
        means[step, :, pl.ds(pl.multiple_of(other, LANES), quarter)] = theirs[:, :quarter].astype(jnp.float32)


def scale_kernel(means, totals, scales):
    tasks, folded, _ = means.shape
    for step in range(tasks):
        total = jnp.sum(totals[step], axis=1, keepdims=True)
        total = total + jnp.concatenate([total[folded // 2 :], total[: folded // 2]], axis=0)
        grand = total * (1.0 / (EXPERTS * FF))
        mean = means[step]
        rounded = (0.2 + 0.7 * mean / (mean + grand)).astype(jnp.bfloat16)
        scales[step] = 1.0 / rounded.astype(jnp.float32)


def merge_kernel(chunks, tasks, aliased, scales, own, *refs):
    half = scales.shape[2]
    layers = own.shape[0]
    columns = 2 * half
    arrived = refs[: len(chunks) * (tasks - 1)]
    out, buf, sems = refs[len(arrived) + aliased :]
    pieces = []
    base = 0
    for place, chunk in enumerate(chunks):
        offset = 0
        for layer, begin, end in chunk:
            for part in range(2):
                low, high = [min(max(at * columns // 8 - part * half, 0), half) for at in (begin, end)]
                if high > low:
                    pieces.append((place, base, layer, part, low, high - low, offset))
                    offset += high - low
        base += offset
    copies = []
    for at, (place, base, layer, part, low, size, offset) in enumerate(pieces):
        row = part * layers + layer

        def body(shift, block):
            narrow = pl.ds(pl.multiple_of(low + shift, LANES), block)
            mine = pl.ds(pl.multiple_of(part * half + low + shift, LANES), block)
            source = pl.ds(pl.multiple_of(offset + shift, LANES), block)
            merged = own[layer, :, mine].astype(jnp.float32) * scales[0, row : row + 1, narrow]
            for step in range(1, tasks):
                other = arrived[place * (tasks - 1) + step - 1][:, source].astype(jnp.float32)
                merged = merged + other * scales[step, row : row + 1, narrow]
            buf[:, pl.ds(pl.multiple_of(base + offset + shift, LANES), block)] = merged.astype(jnp.bfloat16)

        blocks(size, body)
        copies.append(pltpu.make_async_copy(
            buf.at[:, pl.ds(base + offset, size)], out.at[layer, :, pl.ds(part * half + low, size)], sems.at[at]))
        copies[-1].start()
    for copy in copies:
        copy.wait()


def cost(flops, moved):
    return pl.CostEstimate(flops=flops, bytes_accessed=moved, transcendentals=0)


def on_chip(value):
    return pltpu.with_memory_space_constraint(value, pltpu.VMEM)


def merge_all(task_deltas, rank_scores, keep_limits):
    shards, tasks = lax.axis_size("shard"), lax.axis_size("task")
    groups = shards // EXPERTS
    group_bits = groups.bit_length() - 1
    layers, rows, width = task_deltas.shape[1:]
    columns = width // tasks
    half = columns // 2
    block = min(BLOCK, half)
    bf16, f32 = jnp.bfloat16, jnp.float32
    plan = chunk_plan(layers)
    slabs = [pltpu.VMEM((rows, chunk_width(chunk, columns)), bf16) for chunk in plan]

    task_deltas, rank_scores, keep_limits = [
        pltpu.with_memory_space_constraint(value, pltpu.HBM) for value in (task_deltas, rank_scores, keep_limits)
    ]
    first = pl.pallas_call(
        functools.partial(first_kernel, plan[0]),
        out_shape=[slabs[0]] * (tasks - 1),
        in_specs=[HBM] * 3,
        out_specs=[VMEM] * (tasks - 1),
        scratch_shapes=[
            pltpu.SMEM(keep_limits.shape, jnp.int32),
            pltpu.VMEM((tasks - 1, *slabs[0].shape), bf16),
            pltpu.VMEM((tasks - 1, *slabs[0].shape), jnp.int32),
            pltpu.SemaphoreType.DMA((2 * len(plan[0]) * (tasks - 1) + 1,)),
        ],
        compiler_params=pltpu.CompilerParams(vmem_limit_bytes=GRANT),
        cost_estimate=cost(10**6, 6 * rows * columns),
        name="first",
    )(keep_limits, task_deltas, rank_scores)
    arrived = [[shifted(first[step - 1], step) for step in range(1, tasks)]]

    pack = (tasks, 2 * layers, half + LANES)
    copied, packs = pl.pallas_call(
        sums_kernel,
        out_shape=[pltpu.VMEM((layers, rows, width), bf16), pltpu.VMEM(pack, f32)],
        in_specs=[HBM],
        out_specs=[VMEM] * 2,
        scratch_shapes=[pltpu.SemaphoreType.DMA((2 * tasks * half // block,))],
        compiler_params=pltpu.CompilerParams(vmem_limit_bytes=GRANT),
        cost_estimate=cost(10**7, 2 * layers * rows * width),
        name="sums",
    )(task_deltas)

    def masks(places, own_layers):
        chunks = [plan[place] for place in places]
        shapes = [slabs[place] for place in places for _ in range(1, tasks)]
        shapes += [pltpu.VMEM((layers, rows, columns), bf16)] * bool(own_layers)
        pieces = sum(len(chunk) for chunk in chunks) * (tasks - 1) + len(own_layers)
        return pl.pallas_call(
            functools.partial(mask_kernel, chunks, own_layers),
            out_shape=shapes,
            in_specs=[HBM] * 2 + [VMEM],
            out_specs=[VMEM] * len(shapes),
            scratch_shapes=[
                pltpu.SMEM(keep_limits.shape, jnp.int32),
                pltpu.VMEM((pieces, rows, columns), jnp.int32),
                pltpu.SemaphoreType.DMA((pieces + 1,)),
            ],
            compiler_params=pltpu.CompilerParams(vmem_limit_bytes=GRANT),
            cost_estimate=cost(10**7, 6 * pieces * rows * columns),
            name="masks",
        )(keep_limits, rank_scores, on_chip(copied))

    for bit in range(1, group_bits):
        packs = packs + swapped(packs, "shard", bit)
    theirs = swapped(packs, "shard", 0)
    sent = [*masks([1], [])]
    means, totals, *packs = pl.pallas_call(
        pair_kernel,
        out_shape=[pltpu.VMEM((2 * layers, half), f32), pltpu.VMEM((2 * layers, LANES), f32)]
        + [pltpu.VMEM((2 * layers, half // 2 + 2 * LANES), bf16)] * (tasks - 1),
        in_specs=[VMEM] * 2,
        out_specs=[VMEM] * (tasks + 1),
        compiler_params=pltpu.CompilerParams(vmem_limit_bytes=GRANT),
        cost_estimate=cost(10**6, 8 * tasks * layers * half),
        name="pair",
    )(on_chip(packs), on_chip(theirs))
    arrivals = [shifted(packs[step - 1], step) for step in range(1, tasks)]
    arrived.append([shifted(sent[step - 1], step) for step in range(1, tasks)])
    sent += masks([*range(2, len(plan))], [])
    (own,) = masks([], [*range(layers)])
    pairs = []
    for arrival in arrivals:
        pairs += [arrival, swapped(arrival, "shard", 0)]
    last = len(plan) - 1
    for place in range(2, last):
        at = (place - 1) * (tasks - 1)
        arrived.append([shifted(sent[at + step - 1], step) for step in range(1, tasks)])
    exchanged = [swapped(sent[(last - 1) * (tasks - 1) + step - 1], "shard", 0) for step in range(1, tasks)]
    arrived.append([shifted_across(exchanged[step - 1], step) for step in range(1, tasks)])

    totals = pl.pallas_call(
        unpack_kernel,
        out_shape=pltpu.VMEM((tasks, 2 * layers, LANES), f32),
        in_specs=[VMEM] * tasks,
        out_specs=VMEM,
        compiler_params=pltpu.CompilerParams(vmem_limit_bytes=GRANT),
        cost_estimate=cost(10**4, 8 * tasks * layers * LANES),
        name="unpack",
    )(on_chip(totals), *[on_chip(value) for value in arrivals])
    for bit in range(group_bits, shards.bit_length() - 1):
        totals = totals + swapped(totals, "shard", bit)

    means = pl.pallas_call(
        join_kernel,
        out_shape=pltpu.VMEM((tasks, 2 * layers, half), f32),
        in_specs=[VMEM] * (2 * tasks - 1),
        out_specs=VMEM,
        compiler_params=pltpu.CompilerParams(vmem_limit_bytes=GRANT),
        cost_estimate=cost(10**4, 8 * tasks * layers * half),
        name="join",
    )(on_chip(means), *[on_chip(value) for value in pairs])
    scales = pl.pallas_call(
        scale_kernel,
        out_shape=pltpu.VMEM((tasks, 2 * layers, half), f32),
        in_specs=[VMEM] * 2,
        out_specs=VMEM,
        compiler_params=pltpu.CompilerParams(vmem_limit_bytes=GRANT),
        cost_estimate=cost(10**6, 8 * tasks * layers * half),
        name="scale",
    )(on_chip(means), on_chip(totals))

    out = None
    for places in ([*range(last)], [last]):
        chunks = [plan[place] for place in places]
        pieces = [piece for place in places for piece in arrived[place]]
        extra = [] if out is None else [out]
        merged_width = sum(chunk_width(chunk, columns) for chunk in chunks)
        out = pl.pallas_call(
            functools.partial(merge_kernel, chunks, tasks, len(extra)),
            out_shape=jax.ShapeDtypeStruct((layers, rows, columns), bf16),
            in_specs=[VMEM] * (2 + len(pieces)) + [ANY] * len(extra),
            out_specs=ANY,
            scratch_shapes=[
                pltpu.VMEM((rows, merged_width), bf16),
                pltpu.SemaphoreType.DMA((2 * sum(len(chunk) for chunk in chunks),)),
            ],
            input_output_aliases={2 + len(pieces): 0} if extra else {},
            compiler_params=pltpu.CompilerParams(vmem_limit_bytes=GRANT),
            cost_estimate=cost(10**6, 6 * rows * merged_width),
            name="merge",
        )(on_chip(scales), on_chip(own), *[on_chip(piece) for piece in pieces], *extra)
    return out


def solution(mesh):
    return jax.shard_map(
        merge_all,
        mesh=mesh,
        in_specs=(
            P("task", None, "shard", None),
            P("task", None, "shard", None),
            P("task", None, None),
        ),
        out_specs=P(None, "shard", "task"),
        check_vma=False,
    )
```

```python
import functools
import math

import jax
import jax.numpy as jnp
from jax import lax
from jax.experimental import pallas as pl
from jax.experimental.pallas import tpu as pltpu
from jax.sharding import PartitionSpec as P


EXPERTS = 8
FF = 16384
LANES = 128
BLOCK = 2048
CUT = 4
EXTRA = 0
GRANT = 16 * 2**20

ANY = pl.BlockSpec(memory_space=pl.ANY)
HBM = pl.BlockSpec(memory_space=pltpu.HBM)
VMEM = pl.BlockSpec(memory_space=pltpu.VMEM)


def crossed(value, axis, mask):
    return lax.ppermute(value, axis, [(source, source ^ mask) for source in range(lax.axis_size(axis))])


def swapped(value, axis, bit):
    return crossed(value, axis, 1 << bit)


def shifted(value, step):
    size = lax.axis_size("task")
    return lax.ppermute(value, "task", [(source, (source + step) % size) for source in range(size)])


def shifted_across(value, step):
    tasks = lax.axis_size("task")
    pairs = [
        (shard * tasks + source, (shard ^ 1) * tasks + (source + step) % tasks)
        for shard in range(lax.axis_size("shard"))
        for source in range(tasks)
    ]
    return lax.ppermute(value, ("shard", "task"), pairs)


def column_start(step, columns):
    tasks = lax.axis_size("task")
    return lax.rem(lax.axis_index("task") + step, tasks) * columns


def own_expert():
    return lax.axis_index("shard") // (lax.axis_size("shard") // EXPERTS)


def blocks(width, body):
    block = width if width <= 2 * BLOCK else math.gcd(BLOCK, width)
    if block == width:
        body(0, block)
        return

    @pl.loop(0, width // block)
    def _(at):
        body(pl.multiple_of(at * block, block), block)


def chunk_plan(layers):
    last = layers - 1
    middle = [(1, EXTRA, 8), *[(layer, 0, 8) for layer in range(2, last)]]
    return [[(0, 0, 8)], middle, [(last, 0, CUT)], [(last, CUT, 8)]]


def chunk_width(chunk, columns):
    return sum(end - begin for _, begin, end in chunk) * columns // 8


def mask_block(deltas, scores, limit):
    return jnp.where(scores < limit, deltas.astype(jnp.float32), 0.0).astype(jnp.bfloat16)


def first_kernel(chunk, limits, deltas, scores, *refs):
    tasks = lax.axis_size("task")
    outs = refs[: tasks - 1]
    limit_buf, delta_buf, score_buf, sems = refs[tasks - 1 :]
    columns = deltas.shape[3] // tasks
    limit_copy = pltpu.make_async_copy(limits, limit_buf, sems.at[0])
    limit_copy.start()
    work = []
    for step in range(1, tasks):
        offset = 0
        for layer, begin, end in chunk:
            size = (end - begin) * columns // 8
            source = pl.ds(pl.multiple_of(column_start(step, columns) + begin * columns // 8, LANES), size)
            target = pl.ds(offset, size)
            at = 2 * len(work)
            copies = [
                pltpu.make_async_copy(scores.at[0, layer, :, source], score_buf.at[step - 1, :, target], sems.at[at + 1]),
                pltpu.make_async_copy(deltas.at[0, layer, :, source], delta_buf.at[step - 1, :, target], sems.at[at + 2]),
            ]
            for copy in copies:
                copy.start()
            work.append((step, layer, target, copies))
            offset += size
    limit_copy.wait()
    for step, layer, target, copies in work:
        for copy in copies:
            copy.wait()
        limit = limit_buf[0, layer, own_expert()]
        outs[step - 1][:, target] = mask_block(delta_buf[step - 1, :, target], score_buf[step - 1, :, target], limit)


def row_sums(changes):
    values = [change.astype(jnp.float32) for change in changes]
    values = [sum(value[at : at + 8] for at in range(8, value.shape[0], 8)) + value[:8] for value in values]
    if len(values) != 8:
        return jnp.concatenate([jnp.sum(value, axis=0, keepdims=True) for value in values], axis=0)
    lane = lax.broadcasted_iota(jnp.int32, values[0].shape, 0)
    for shift in (4, 2, 1):
        low = lane % (2 * shift) < shift
        values = [
            jnp.where(low, one + pltpu.roll(one, 8 - shift, 0), two + pltpu.roll(two, shift, 0))
            for one, two in zip(values[:shift], values[shift:])
        ]
    return values[0]


def sums_kernel(deltas, copied, packs, sems):
    tasks, folded, packed = packs.shape
    half = packed - LANES
    layers, rows, _ = copied.shape
    columns = 2 * half
    block = min(BLOCK, half)
    places = half // block
    groups = lax.axis_size("shard") // EXPERTS
    work = [(step, place) for step in range(tasks) for place in range(places)]
    copies = []
    sources = []
    for step, place in work:
        start = column_start(step, columns) + place * block
        sources.append([pl.ds(pl.multiple_of(start + part * half, LANES), block) for part in range(2)])
        copies.append([
            pltpu.make_async_copy(deltas.at[0, :, :, source], copied.at[:, :, source], sems.at[2 * len(copies) + part])
            for part, source in enumerate(sources[-1])
        ])
        for copy in copies[-1]:
            copy.start()
    totals = jnp.zeros((folded, LANES), jnp.float32)
    for at, (step, place) in enumerate(work):
        for copy in copies[at]:
            copy.wait()
        sums = row_sums([jnp.abs(copied[layer, :, source]) for source in sources[at] for layer in range(layers)])
        means = sums * (1.0 / (rows * groups))
        packs[step, :, place * block : (place + 1) * block] = means
        for tile in range(0, block, LANES):
            totals = totals + means[:, tile : tile + LANES]
    for step in range(tasks):
        packs[step, :, half:] = totals


def store_split(pack, totals):
    layers = totals.shape[0] // 2
    folded = totals[:layers] + totals[layers:]
    high = folded.astype(jnp.bfloat16).astype(jnp.float32)
    pack[:, pack.shape[1] - LANES :] = jnp.concatenate([high, folded - high], axis=0).astype(jnp.bfloat16)


def mask_kernel(chunks, own_layers, limits, scores, copied, *refs):
    tasks = lax.axis_size("task")
    _, _, width = copied.shape
    columns = width // tasks
    count = len(chunks) * (tasks - 1)
    sent, refs = refs[:count], refs[count:]
    if own_layers:
        own, refs = refs[0], refs[1:]
    limit_buf, score_buf, sems = refs
    limit_copy = pltpu.make_async_copy(limits, limit_buf, sems.at[0])
    limit_copy.start()
    work = []
    for at, chunk in enumerate(chunks):
        for step in range(1, tasks):
            offset = 0
            for layer, begin, end in chunk:
                size = (end - begin) * columns // 8
                work.append((sent[at * (tasks - 1) + step - 1], offset, layer, step, begin * columns // 8, size))
                offset += size
    work += [(own.at[layer], 0, layer, 0, 0, columns) for layer in own_layers]
    copies = []
    for at, (_, _, layer, step, begin, size) in enumerate(work):
        source = pl.ds(pl.multiple_of(column_start(step, columns) + begin, LANES), size)
        copies.append(pltpu.make_async_copy(scores.at[0, layer, :, source], score_buf.at[at, :, :size], sems.at[at + 1]))
        copies[-1].start()
    limit_copy.wait()
    for at, (target, offset, layer, step, begin, size) in enumerate(work):
        start = column_start(step, columns) + begin
        limit = limit_buf[0, layer, own_expert()]
        copies[at].wait()

        def body(place, block):
            change = copied[layer, :, pl.ds(pl.multiple_of(start + place, LANES), block)]
            kept = mask_block(change, score_buf[at, :, pl.ds(place, block)], limit)
            target[:, pl.ds(pl.multiple_of(offset + place, LANES), block)] = kept

        blocks(size, body)


def slot_lanes(width):
    return pl.ds(pl.multiple_of(lax.rem(lax.axis_index("shard"), 2) * width, LANES), width)


def pair_kernel(mine, theirs, means, totals, *packs):
    tasks, _, packed = mine.shape
    half = packed - LANES
    means[...] = mine[0, :, :half] + theirs[0, :, :half]
    total = mine[0, :, half:] + theirs[0, :, half:]
    totals[...] = total
    for step in range(1, tasks):
        picked = mine[step, :, slot_lanes(half // 2)] + theirs[step, :, slot_lanes(half // 2)]
        packs[step - 1][:, : half // 2] = picked.astype(jnp.bfloat16)
        store_split(packs[step - 1], total)


def unpack_kernel(own_totals, *refs):
    arrivals, totals = refs[:-1], refs[-1]
    totals[0] = own_totals[...]
    for step, arrival in enumerate(arrivals, 1):
        totals[step] = arrival[:, arrival.shape[1] - LANES :].astype(jnp.float32)


def join_kernel(own_means, *refs):
    pairs, means = refs[:-1], refs[-1]
    quarter = means.shape[2] // 2
    means[0] = own_means[...]
    other = lax.rem(lax.axis_index("shard") + 1, 2) * quarter
    for step in range(1, means.shape[0]):
        mine, theirs = pairs[2 * step - 2 : 2 * step]
        means[step, :, slot_lanes(quarter)] = mine[:, :quarter].astype(jnp.float32)
        means[step, :, pl.ds(pl.multiple_of(other, LANES), quarter)] = theirs[:, :quarter].astype(jnp.float32)


def scale_kernel(means, totals, scales):
    tasks, folded, _ = means.shape
    for step in range(tasks):
        total = jnp.sum(totals[step], axis=1, keepdims=True)
        total = total + jnp.concatenate([total[folded // 2 :], total[: folded // 2]], axis=0)
        grand = total * (1.0 / (EXPERTS * FF))
        mean = means[step]
        rounded = (0.2 + 0.7 * mean / (mean + grand)).astype(jnp.bfloat16)
        scales[step] = 1.0 / rounded.astype(jnp.float32)


def merge_kernel(chunks, tasks, aliased, scales, own, *refs):
    half = scales.shape[2]
    layers = own.shape[0]
    columns = 2 * half
    arrived = refs[: len(chunks) * (tasks - 1)]
    out, buf, sems = refs[len(arrived) + aliased :]
    pieces = []
    base = 0
    for place, chunk in enumerate(chunks):
        offset = 0
        for layer, begin, end in chunk:
            for part in range(2):
                low, high = [min(max(at * columns // 8 - part * half, 0), half) for at in (begin, end)]
                if high > low:
                    pieces.append((place, base, layer, part, low, high - low, offset))
                    offset += high - low
        base += offset
    copies = []
    for at, (place, base, layer, part, low, size, offset) in enumerate(pieces):
        row = part * layers + layer

        def body(shift, block):
            narrow = pl.ds(pl.multiple_of(low + shift, LANES), block)
            mine = pl.ds(pl.multiple_of(part * half + low + shift, LANES), block)
            source = pl.ds(pl.multiple_of(offset + shift, LANES), block)
            merged = own[layer, :, mine].astype(jnp.float32) * scales[0, row : row + 1, narrow]
            for step in range(1, tasks):
                other = arrived[place * (tasks - 1) + step - 1][:, source].astype(jnp.float32)
                merged = merged + other * scales[step, row : row + 1, narrow]
            buf[:, pl.ds(pl.multiple_of(base + offset + shift, LANES), block)] = merged.astype(jnp.bfloat16)

        blocks(size, body)
        copies.append(pltpu.make_async_copy(
            buf.at[:, pl.ds(base + offset, size)], out.at[layer, :, pl.ds(part * half + low, size)], sems.at[at]))
        copies[-1].start()
    for copy in copies:
        copy.wait()


def cost(flops, moved):
    return pl.CostEstimate(flops=flops, bytes_accessed=moved, transcendentals=0)


def on_chip(value):
    return pltpu.with_memory_space_constraint(value, pltpu.VMEM)


def merge_all(task_deltas, rank_scores, keep_limits):
    shards, tasks = lax.axis_size("shard"), lax.axis_size("task")
    groups = shards // EXPERTS
    group_bits = groups.bit_length() - 1
    layers, rows, width = task_deltas.shape[1:]
    columns = width // tasks
    half = columns // 2
    block = min(BLOCK, half)
    bf16, f32 = jnp.bfloat16, jnp.float32
    plan = chunk_plan(layers)
    slabs = [pltpu.VMEM((rows, chunk_width(chunk, columns)), bf16) for chunk in plan]

    task_deltas, rank_scores, keep_limits = [
        pltpu.with_memory_space_constraint(value, pltpu.HBM) for value in (task_deltas, rank_scores, keep_limits)
    ]
    first = pl.pallas_call(
        functools.partial(first_kernel, plan[0]),
        out_shape=[slabs[0]] * (tasks - 1),
        in_specs=[HBM] * 3,
        out_specs=[VMEM] * (tasks - 1),
        scratch_shapes=[
            pltpu.SMEM(keep_limits.shape, jnp.int32),
            pltpu.VMEM((tasks - 1, *slabs[0].shape), bf16),
            pltpu.VMEM((tasks - 1, *slabs[0].shape), jnp.int32),
            pltpu.SemaphoreType.DMA((2 * len(plan[0]) * (tasks - 1) + 1,)),
        ],
        compiler_params=pltpu.CompilerParams(vmem_limit_bytes=GRANT),
        cost_estimate=cost(10**6, 6 * rows * columns),
        name="first",
    )(keep_limits, task_deltas, rank_scores)
    arrived = [[shifted(first[step - 1], step) for step in range(1, tasks)]]

    pack = (tasks, 2 * layers, half + LANES)
    copied, packs = pl.pallas_call(
        sums_kernel,
        out_shape=[pltpu.VMEM((layers, rows, width), bf16), pltpu.VMEM(pack, f32)],
        in_specs=[HBM],
        out_specs=[VMEM] * 2,
        scratch_shapes=[pltpu.SemaphoreType.DMA((2 * tasks * half // block,))],
        compiler_params=pltpu.CompilerParams(vmem_limit_bytes=GRANT),
        cost_estimate=cost(10**7, 2 * layers * rows * width),
        name="sums",
    )(task_deltas)

    def masks(places, own_layers):
        chunks = [plan[place] for place in places]
        shapes = [slabs[place] for place in places for _ in range(1, tasks)]
        shapes += [pltpu.VMEM((layers, rows, columns), bf16)] * bool(own_layers)
        pieces = sum(len(chunk) for chunk in chunks) * (tasks - 1) + len(own_layers)
        return pl.pallas_call(
            functools.partial(mask_kernel, chunks, own_layers),
            out_shape=shapes,
            in_specs=[HBM] * 2 + [VMEM],
            out_specs=[VMEM] * len(shapes),
            scratch_shapes=[
                pltpu.SMEM(keep_limits.shape, jnp.int32),
                pltpu.VMEM((pieces, rows, columns), jnp.int32),
                pltpu.SemaphoreType.DMA((pieces + 1,)),
            ],
            compiler_params=pltpu.CompilerParams(vmem_limit_bytes=GRANT),
            cost_estimate=cost(10**7, 6 * pieces * rows * columns),
            name="masks",
        )(keep_limits, rank_scores, on_chip(copied))

    for bit in range(1, group_bits):
        packs = packs + swapped(packs, "shard", bit)
    theirs = swapped(packs, "shard", 0)
    sent = [*masks([1], [])]
    means, totals, *packs = pl.pallas_call(
        pair_kernel,
        out_shape=[pltpu.VMEM((2 * layers, half), f32), pltpu.VMEM((2 * layers, LANES), f32)]
        + [pltpu.VMEM((2 * layers, half // 2 + LANES), bf16)] * (tasks - 1),
        in_specs=[VMEM] * 2,
        out_specs=[VMEM] * (tasks + 1),
        compiler_params=pltpu.CompilerParams(vmem_limit_bytes=GRANT),
        cost_estimate=cost(10**6, 8 * tasks * layers * half),
        name="pair",
    )(on_chip(packs), on_chip(theirs))
    arrivals = [shifted(packs[step - 1], step) for step in range(1, tasks)]
    arrived.append([shifted(sent[step - 1], step) for step in range(1, tasks)])
    sent += masks([*range(2, len(plan))], [])
    (own,) = masks([], [*range(layers)])
    pairs = []
    for arrival in arrivals:
        pairs += [arrival, swapped(arrival, "shard", 0)]
    last = len(plan) - 1
    for place in range(2, last):
        at = (place - 1) * (tasks - 1)
        arrived.append([shifted(sent[at + step - 1], step) for step in range(1, tasks)])
    exchanged = [swapped(sent[(last - 1) * (tasks - 1) + step - 1], "shard", 0) for step in range(1, tasks)]
    arrived.append([shifted_across(exchanged[step - 1], step) for step in range(1, tasks)])

    totals = pl.pallas_call(
        unpack_kernel,
        out_shape=pltpu.VMEM((tasks, 2 * layers, LANES), f32),
        in_specs=[VMEM] * tasks,
        out_specs=VMEM,
        compiler_params=pltpu.CompilerParams(vmem_limit_bytes=GRANT),
        cost_estimate=cost(10**4, 8 * tasks * layers * LANES),
        name="unpack",
    )(on_chip(totals), *[on_chip(value) for value in arrivals])
    for bit in range(group_bits, shards.bit_length() - 1):
        totals = totals + swapped(totals, "shard", bit)

    means = pl.pallas_call(
        join_kernel,
        out_shape=pltpu.VMEM((tasks, 2 * layers, half), f32),
        in_specs=[VMEM] * (2 * tasks - 1),
        out_specs=VMEM,
        compiler_params=pltpu.CompilerParams(vmem_limit_bytes=GRANT),
        cost_estimate=cost(10**4, 8 * tasks * layers * half),
        name="join",
    )(on_chip(means), *[on_chip(value) for value in pairs])
    scales = pl.pallas_call(
        scale_kernel,
        out_shape=pltpu.VMEM((tasks, 2 * layers, half), f32),
        in_specs=[VMEM] * 2,
        out_specs=VMEM,
        compiler_params=pltpu.CompilerParams(vmem_limit_bytes=GRANT),
        cost_estimate=cost(10**6, 8 * tasks * layers * half),
        name="scale",
    )(on_chip(means), on_chip(totals))

    out = None
    for places in ([*range(last)], [last]):
        chunks = [plan[place] for place in places]
        pieces = [piece for place in places for piece in arrived[place]]
        extra = [] if out is None else [out]
        merged_width = sum(chunk_width(chunk, columns) for chunk in chunks)
        out = pl.pallas_call(
            functools.partial(merge_kernel, chunks, tasks, len(extra)),
            out_shape=jax.ShapeDtypeStruct((layers, rows, columns), bf16),
            in_specs=[VMEM] * (2 + len(pieces)) + [ANY] * len(extra),
            out_specs=ANY,
            scratch_shapes=[
                pltpu.VMEM((rows, merged_width), bf16),
                pltpu.SemaphoreType.DMA((2 * sum(len(chunk) for chunk in chunks),)),
            ],
            input_output_aliases={2 + len(pieces): 0} if extra else {},
            compiler_params=pltpu.CompilerParams(vmem_limit_bytes=GRANT),
            cost_estimate=cost(10**6, 6 * rows * merged_width),
            name="merge",
        )(on_chip(scales), on_chip(own), *[on_chip(piece) for piece in pieces], *extra)
    return out


def solution(mesh):
    return jax.shard_map(
        merge_all,
        mesh=mesh,
        in_specs=(
            P("task", None, "shard", None),
            P("task", None, "shard", None),
            P("task", None, None),
        ),
        out_specs=P(None, "shard", "task"),
        check_vma=False,
    )
```

```python
import functools
import math

import jax
import jax.numpy as jnp
from jax import lax
from jax.experimental import pallas as pl
from jax.experimental.pallas import tpu as pltpu
from jax.sharding import PartitionSpec as P


EXPERTS = 8
FF = 16384
LANES = 128
BLOCK = 2048
CUT = 4
EXTRA = 0
GRANT = 16 * 2**20

ANY = pl.BlockSpec(memory_space=pl.ANY)
HBM = pl.BlockSpec(memory_space=pltpu.HBM)
VMEM = pl.BlockSpec(memory_space=pltpu.VMEM)


def crossed(value, axis, mask):
    return lax.ppermute(value, axis, [(source, source ^ mask) for source in range(lax.axis_size(axis))])


def swapped(value, axis, bit):
    return crossed(value, axis, 1 << bit)


def shifted(value, step):
    size = lax.axis_size("task")
    return lax.ppermute(value, "task", [(source, (source + step) % size) for source in range(size)])


def shifted_across(value, step):
    tasks = lax.axis_size("task")
    pairs = [
        (shard * tasks + source, (shard ^ 1) * tasks + (source + step) % tasks)
        for shard in range(lax.axis_size("shard"))
        for source in range(tasks)
    ]
    return lax.ppermute(value, ("shard", "task"), pairs)


def column_start(step, columns):
    tasks = lax.axis_size("task")
    return lax.rem(lax.axis_index("task") + step, tasks) * columns


def own_expert():
    return lax.axis_index("shard") // (lax.axis_size("shard") // EXPERTS)


def blocks(width, body):
    block = width if width <= 2 * BLOCK else math.gcd(BLOCK, width)
    if block == width:
        body(0, block)
        return

    @pl.loop(0, width // block)
    def _(at):
        body(pl.multiple_of(at * block, block), block)


def chunk_plan(layers):
    last = layers - 1
    middle = [(1, EXTRA, 8), *[(layer, 0, 8) for layer in range(2, last)]]
    return [[(0, 0, 8)], middle, [(last, 0, CUT)], [(last, CUT, 8)]]


def chunk_width(chunk, columns):
    return sum(end - begin for _, begin, end in chunk) * columns // 8


def mask_block(deltas, scores, limit):
    return jnp.where(scores < limit, deltas.astype(jnp.float32), 0.0).astype(jnp.bfloat16)


def first_kernel(chunk, limits, deltas, scores, *refs):
    tasks = lax.axis_size("task")
    outs = refs[: tasks - 1]
    limit_buf, delta_buf, score_buf, sems = refs[tasks - 1 :]
    columns = deltas.shape[3] // tasks
    limit_copy = pltpu.make_async_copy(limits, limit_buf, sems.at[0])
    limit_copy.start()
    work = []
    for step in range(1, tasks):
        offset = 0
        for layer, begin, end in chunk:
            size = (end - begin) * columns // 8
            source = pl.ds(pl.multiple_of(column_start(step, columns) + begin * columns // 8, LANES), size)
            target = pl.ds(offset, size)
            at = 2 * len(work)
            copies = [
                pltpu.make_async_copy(scores.at[0, layer, :, source], score_buf.at[step - 1, :, target], sems.at[at + 1]),
                pltpu.make_async_copy(deltas.at[0, layer, :, source], delta_buf.at[step - 1, :, target], sems.at[at + 2]),
            ]
            for copy in copies:
                copy.start()
            work.append((step, layer, target, copies))
            offset += size
    limit_copy.wait()
    for step, layer, target, copies in work:
        for copy in copies:
            copy.wait()
        limit = limit_buf[0, layer, own_expert()]
        outs[step - 1][:, target] = mask_block(delta_buf[step - 1, :, target], score_buf[step - 1, :, target], limit)


def row_sums(changes):
    values = [change.astype(jnp.float32) for change in changes]
    values = [sum(value[at : at + 8] for at in range(8, value.shape[0], 8)) + value[:8] for value in values]
    if len(values) != 8:
        return jnp.concatenate([jnp.sum(value, axis=0, keepdims=True) for value in values], axis=0)
    lane = lax.broadcasted_iota(jnp.int32, values[0].shape, 0)
    for shift in (4, 2, 1):
        low = lane % (2 * shift) < shift
        values = [
            jnp.where(low, one + pltpu.roll(one, 8 - shift, 0), two + pltpu.roll(two, shift, 0))
            for one, two in zip(values[:shift], values[shift:])
        ]
    return values[0]


def sums_kernel(deltas, copied, packs, sems):
    tasks, folded, packed = packs.shape
    half = packed - LANES
    layers, rows, _ = copied.shape
    columns = 2 * half
    block = min(BLOCK, half)
    places = half // block
    groups = lax.axis_size("shard") // EXPERTS
    work = [(step, place) for step in range(tasks) for place in range(places)]
    copies = []
    sources = []
    for step, place in work:
        start = column_start(step, columns) + place * block
        sources.append([pl.ds(pl.multiple_of(start + part * half, LANES), block) for part in range(2)])
        copies.append([
            pltpu.make_async_copy(deltas.at[0, :, :, source], copied.at[:, :, source], sems.at[2 * len(copies) + part])
            for part, source in enumerate(sources[-1])
        ])
        for copy in copies[-1]:
            copy.start()
    totals = jnp.zeros((folded, LANES), jnp.float32)
    for at, (step, place) in enumerate(work):
        for copy in copies[at]:
            copy.wait()
        sums = row_sums([jnp.abs(copied[layer, :, source]) for source in sources[at] for layer in range(layers)])
        means = sums * (1.0 / (rows * groups))
        packs[step, :, place * block : (place + 1) * block] = means
        for tile in range(0, block, LANES):
            totals = totals + means[:, tile : tile + LANES]
    for step in range(tasks):
        packs[step, :, half:] = totals


def store_split(pack, totals):
    layers = totals.shape[0] // 2
    folded = totals[:layers] + totals[layers:]
    high = folded.astype(jnp.bfloat16).astype(jnp.float32)
    pack[:, pack.shape[1] - LANES :] = jnp.concatenate([high, folded - high], axis=0).astype(jnp.bfloat16)


def mask_kernel(chunks, own_layers, limits, scores, copied, *refs):
    tasks = lax.axis_size("task")
    _, _, width = copied.shape
    columns = width // tasks
    count = len(chunks) * (tasks - 1)
    sent, refs = refs[:count], refs[count:]
    if own_layers:
        own, refs = refs[0], refs[1:]
    limit_buf, score_buf, sems = refs
    limit_copy = pltpu.make_async_copy(limits, limit_buf, sems.at[0])
    limit_copy.start()
    work = []
    for at, chunk in enumerate(chunks):
        for step in range(1, tasks):
            offset = 0
            for layer, begin, end in chunk:
                size = (end - begin) * columns // 8
                work.append((sent[at * (tasks - 1) + step - 1], offset, layer, step, begin * columns // 8, size))
                offset += size
    work += [(own.at[layer], 0, layer, 0, 0, columns) for layer in own_layers]
    copies = []
    for at, (_, _, layer, step, begin, size) in enumerate(work):
        source = pl.ds(pl.multiple_of(column_start(step, columns) + begin, LANES), size)
        copies.append(pltpu.make_async_copy(scores.at[0, layer, :, source], score_buf.at[at, :, :size], sems.at[at + 1]))
        copies[-1].start()
    limit_copy.wait()
    for at, (target, offset, layer, step, begin, size) in enumerate(work):
        start = column_start(step, columns) + begin
        limit = limit_buf[0, layer, own_expert()]
        copies[at].wait()

        def body(place, block):
            change = copied[layer, :, pl.ds(pl.multiple_of(start + place, LANES), block)]
            kept = mask_block(change, score_buf[at, :, pl.ds(place, block)], limit)
            target[:, pl.ds(pl.multiple_of(offset + place, LANES), block)] = kept

        blocks(size, body)


def slot_lanes(width):
    return pl.ds(pl.multiple_of(lax.rem(lax.axis_index("shard"), 2) * width, LANES), width)


def pair_kernel(mine, theirs, means, totals, *packs):
    tasks, _, packed = mine.shape
    half = packed - LANES
    means[...] = mine[0, :, :half] + theirs[0, :, :half]
    total = mine[0, :, half:] + theirs[0, :, half:]
    totals[...] = total
    for step in range(1, tasks):
        picked = mine[step, :, slot_lanes(half // 2)] + theirs[step, :, slot_lanes(half // 2)]
        packs[step - 1][:, : half // 2] = picked.astype(jnp.bfloat16)
        store_split(packs[step - 1], total)


def unpack_kernel(own_totals, *refs):
    arrivals, totals = refs[:-1], refs[-1]
    totals[0] = own_totals[...]
    for step, arrival in enumerate(arrivals, 1):
        totals[step] = arrival[:, arrival.shape[1] - LANES :].astype(jnp.float32)


def join_kernel(own_means, *refs):
    pairs, means = refs[:-1], refs[-1]
    quarter = means.shape[2] // 2
    means[0] = own_means[...]
    other = lax.rem(lax.axis_index("shard") + 1, 2) * quarter
    for step in range(1, means.shape[0]):
        mine, theirs = pairs[2 * step - 2 : 2 * step]
        means[step, :, slot_lanes(quarter)] = mine[:, :quarter].astype(jnp.float32)
        means[step, :, pl.ds(pl.multiple_of(other, LANES), quarter)] = theirs[:, :quarter].astype(jnp.float32)


def scale_kernel(means, totals, scales):
    tasks, folded, _ = means.shape
    for step in range(tasks):
        total = jnp.sum(totals[step], axis=1, keepdims=True)
        total = total + jnp.concatenate([total[folded // 2 :], total[: folded // 2]], axis=0)
        grand = total * (1.0 / (EXPERTS * FF))
        mean = means[step]
        rounded = (0.2 + 0.7 * mean / (mean + grand)).astype(jnp.bfloat16)
        scales[step] = 1.0 / rounded.astype(jnp.float32)


def merge_kernel(chunks, tasks, aliased, scales, own, *refs):
    half = scales.shape[2]
    layers = own.shape[0]
    columns = 2 * half
    arrived = refs[: len(chunks) * (tasks - 1)]
    out, buf, sems = refs[len(arrived) + aliased :]
    pieces = []
    base = 0
    for place, chunk in enumerate(chunks):
        offset = 0
        for layer, begin, end in chunk:
            for part in range(2):
                low, high = [min(max(at * columns // 8 - part * half, 0), half) for at in (begin, end)]
                size = (high - low) // (4 if len(chunks) == 1 else 1)
                for start in range(low, high, size or 1):
                    pieces.append((place, base, layer, part, start, size, offset))
                    offset += size
        base += offset
    copies = []
    for at, (place, base, layer, part, low, size, offset) in enumerate(pieces):
        row = part * layers + layer

        def body(shift, block):
            narrow = pl.ds(pl.multiple_of(low + shift, LANES), block)
            mine = pl.ds(pl.multiple_of(part * half + low + shift, LANES), block)
            source = pl.ds(pl.multiple_of(offset + shift, LANES), block)
            merged = own[layer, :, mine].astype(jnp.float32) * scales[0, row : row + 1, narrow]
            for step in range(1, tasks):
                other = arrived[place * (tasks - 1) + step - 1][:, source].astype(jnp.float32)
                merged = merged + other * scales[step, row : row + 1, narrow]
            buf[:, pl.ds(pl.multiple_of(base + offset + shift, LANES), block)] = merged.astype(jnp.bfloat16)

        blocks(size, body)
        copies.append(pltpu.make_async_copy(
            buf.at[:, pl.ds(base + offset, size)], out.at[layer, :, pl.ds(part * half + low, size)], sems.at[at]))
        copies[-1].start()
    for copy in copies:
        copy.wait()


def cost(flops, moved):
    return pl.CostEstimate(flops=flops, bytes_accessed=moved, transcendentals=0)


def on_chip(value):
    return pltpu.with_memory_space_constraint(value, pltpu.VMEM)


def merge_all(task_deltas, rank_scores, keep_limits):
    shards, tasks = lax.axis_size("shard"), lax.axis_size("task")
    groups = shards // EXPERTS
    group_bits = groups.bit_length() - 1
    layers, rows, width = task_deltas.shape[1:]
    columns = width // tasks
    half = columns // 2
    block = min(BLOCK, half)
    bf16, f32 = jnp.bfloat16, jnp.float32
    plan = chunk_plan(layers)
    slabs = [pltpu.VMEM((rows, chunk_width(chunk, columns)), bf16) for chunk in plan]

    task_deltas, rank_scores, keep_limits = [
        pltpu.with_memory_space_constraint(value, pltpu.HBM) for value in (task_deltas, rank_scores, keep_limits)
    ]
    first = pl.pallas_call(
        functools.partial(first_kernel, plan[0]),
        out_shape=[slabs[0]] * (tasks - 1),
        in_specs=[HBM] * 3,
        out_specs=[VMEM] * (tasks - 1),
        scratch_shapes=[
            pltpu.SMEM(keep_limits.shape, jnp.int32),
            pltpu.VMEM((tasks - 1, *slabs[0].shape), bf16),
            pltpu.VMEM((tasks - 1, *slabs[0].shape), jnp.int32),
            pltpu.SemaphoreType.DMA((2 * len(plan[0]) * (tasks - 1) + 1,)),
        ],
        compiler_params=pltpu.CompilerParams(vmem_limit_bytes=GRANT),
        cost_estimate=cost(10**6, 6 * rows * columns),
        name="first",
    )(keep_limits, task_deltas, rank_scores)
    arrived = [[shifted(first[step - 1], step) for step in range(1, tasks)]]

    pack = (tasks, 2 * layers, half + LANES)
    copied, packs = pl.pallas_call(
        sums_kernel,
        out_shape=[pltpu.VMEM((layers, rows, width), bf16), pltpu.VMEM(pack, f32)],
        in_specs=[HBM],
        out_specs=[VMEM] * 2,
        scratch_shapes=[pltpu.SemaphoreType.DMA((2 * tasks * half // block,))],
        compiler_params=pltpu.CompilerParams(vmem_limit_bytes=GRANT),
        cost_estimate=cost(10**7, 2 * layers * rows * width),
        name="sums",
    )(task_deltas)

    def masks(places, own_layers):
        chunks = [plan[place] for place in places]
        shapes = [slabs[place] for place in places for _ in range(1, tasks)]
        shapes += [pltpu.VMEM((layers, rows, columns), bf16)] * bool(own_layers)
        pieces = sum(len(chunk) for chunk in chunks) * (tasks - 1) + len(own_layers)
        return pl.pallas_call(
            functools.partial(mask_kernel, chunks, own_layers),
            out_shape=shapes,
            in_specs=[HBM] * 2 + [VMEM],
            out_specs=[VMEM] * len(shapes),
            scratch_shapes=[
                pltpu.SMEM(keep_limits.shape, jnp.int32),
                pltpu.VMEM((pieces, rows, columns), jnp.int32),
                pltpu.SemaphoreType.DMA((pieces + 1,)),
            ],
            compiler_params=pltpu.CompilerParams(vmem_limit_bytes=GRANT),
            cost_estimate=cost(10**7, 6 * pieces * rows * columns),
            name="masks",
        )(keep_limits, rank_scores, on_chip(copied))

    for bit in range(1, group_bits):
        packs = packs + swapped(packs, "shard", bit)
    theirs = swapped(packs, "shard", 0)
    sent = [*masks([1], [])]
    means, totals, *packs = pl.pallas_call(
        pair_kernel,
        out_shape=[pltpu.VMEM((2 * layers, half), f32), pltpu.VMEM((2 * layers, LANES), f32)]
        + [pltpu.VMEM((2 * layers, half // 2 + LANES), bf16)] * (tasks - 1),
        in_specs=[VMEM] * 2,
        out_specs=[VMEM] * (tasks + 1),
        compiler_params=pltpu.CompilerParams(vmem_limit_bytes=GRANT),
        cost_estimate=cost(10**6, 8 * tasks * layers * half),
        name="pair",
    )(on_chip(packs), on_chip(theirs))
    arrivals = [shifted(packs[step - 1], step) for step in range(1, tasks)]
    arrived.append([shifted(sent[step - 1], step) for step in range(1, tasks)])
    sent += masks([*range(2, len(plan))], [])
    (own,) = masks([], [*range(layers)])
    pairs = []
    for arrival in arrivals:
        pairs += [arrival, swapped(arrival, "shard", 0)]
    last = len(plan) - 1
    for place in range(2, last):
        at = (place - 1) * (tasks - 1)
        arrived.append([shifted(sent[at + step - 1], step) for step in range(1, tasks)])
    exchanged = [swapped(sent[(last - 1) * (tasks - 1) + step - 1], "shard", 0) for step in range(1, tasks)]
    arrived.append([shifted_across(exchanged[step - 1], step) for step in range(1, tasks)])

    totals = pl.pallas_call(
        unpack_kernel,
        out_shape=pltpu.VMEM((tasks, 2 * layers, LANES), f32),
        in_specs=[VMEM] * tasks,
        out_specs=VMEM,
        compiler_params=pltpu.CompilerParams(vmem_limit_bytes=GRANT),
        cost_estimate=cost(10**4, 8 * tasks * layers * LANES),
        name="unpack",
    )(on_chip(totals), *[on_chip(value) for value in arrivals])
    for bit in range(group_bits, shards.bit_length() - 1):
        totals = totals + swapped(totals, "shard", bit)

    means = pl.pallas_call(
        join_kernel,
        out_shape=pltpu.VMEM((tasks, 2 * layers, half), f32),
        in_specs=[VMEM] * (2 * tasks - 1),
        out_specs=VMEM,
        compiler_params=pltpu.CompilerParams(vmem_limit_bytes=GRANT),
        cost_estimate=cost(10**4, 8 * tasks * layers * half),
        name="join",
    )(on_chip(means), *[on_chip(value) for value in pairs])
    scales = pl.pallas_call(
        scale_kernel,
        out_shape=pltpu.VMEM((tasks, 2 * layers, half), f32),
        in_specs=[VMEM] * 2,
        out_specs=VMEM,
        compiler_params=pltpu.CompilerParams(vmem_limit_bytes=GRANT),
        cost_estimate=cost(10**6, 8 * tasks * layers * half),
        name="scale",
    )(on_chip(means), on_chip(totals))

    out = None
    for places in ([*range(last)], [last]):
        chunks = [plan[place] for place in places]
        pieces = [piece for place in places for piece in arrived[place]]
        extra = [] if out is None else [out]
        merged_width = sum(chunk_width(chunk, columns) for chunk in chunks)
        out = pl.pallas_call(
            functools.partial(merge_kernel, chunks, tasks, len(extra)),
            out_shape=jax.ShapeDtypeStruct((layers, rows, columns), bf16),
            in_specs=[VMEM] * (2 + len(pieces)) + [ANY] * len(extra),
            out_specs=ANY,
            scratch_shapes=[
                pltpu.VMEM((rows, merged_width), bf16),
                pltpu.SemaphoreType.DMA((max(4, 2 * sum(len(chunk) for chunk in chunks)),)),
            ],
            input_output_aliases={2 + len(pieces): 0} if extra else {},
            compiler_params=pltpu.CompilerParams(vmem_limit_bytes=GRANT),
            cost_estimate=cost(10**6, 6 * rows * merged_width),
            name="merge",
        )(on_chip(scales), on_chip(own), *[on_chip(piece) for piece in pieces], *extra)
    return out


def solution(mesh):
    return jax.shard_map(
        merge_all,
        mesh=mesh,
        in_specs=(
            P("task", None, "shard", None),
            P("task", None, "shard", None),
            P("task", None, None),
        ),
        out_specs=P(None, "shard", "task"),
        check_vma=False,
    )
```
